256 devices in a mesh: event: 4 (over y, x), draw: 32 (over z), bin: 2 (over core).
Axes of the slice: x: 2, y: 2, z: 32, core: 2. Of those that a mesh axis runs over, the one named last changes fastest.
The devices are a block of a 4x8x32 slice.
Arguments:
- fine_cross: float32 [12, 2, 8192], P('event', None, 'draw'), parts along dimension 0, may hold values from -0.15 to 0.15
- fine_power: float32 [12, 8192], P('event', 'draw'), parts along dimension 0, may hold values from 0.000125 to 0.005
- bin_widths: int32 [512], P('event'), parts along dimension 0, may hold values from 1 to 128, 8192 in all
- log_amps: float32 [12, 32768], P('event', 'draw'), parts along dimension 0, may hold values from -0.5 to 0.5
- delays: float32 [12, 32768], P('event', 'draw'), parts along dimension 0, may hold values from -1.5 to 1.5
- phases: float32 [131072], P(('event', 'draw')), parts along dimension 0, may hold values from -3.140625 to 3.140625
- chirps: float32 [131072], P(('event', 'draw')), parts along dimension 0, may hold values from -8 to 8
- proposal_log: float32 [131072], P(('event', 'draw')), parts along dimension 0, may hold values from -100 to 130
Outputs:
- log_weights: float32 [131072], P(('event', 'draw')), parts along dimension 0
- log_evidence: float32 [4], P('event'), parts along dimension 0
The draws below stay inside these ranges and needn't reach their ends.
There are 4 independent parts, one for each index of `event`. The reference program is written for one: setup_inputs(seed, part) draws one part's arguments, and reference() takes and returns one part's arrays. A program takes and returns all parts, laid end to end along the dimension named above; each array names one. Nothing has to cross between parts.
Inputs may be any that keep to these rules, and one draw needn't show every extreme that they name: `bin_widths`: the widths of an event sum to 8192; each is 1 to 128 and one is exactly 128.
All inputs are finite; a program needn't handle non-finite values.
Results may differ from the reference program's by a relative error of at most 0.00016.
Values sent between devices are 32-bit elements; how exact they have to be, the bound alone decides.
No kernel may reach another device: no remote copies, remote signals or barrier semaphores. Data moves between devices by JAX's collectives and lax.ppermute only.
A program may use at most 64 MiB of HBM per device.

```python
import math
import jax
import jax.numpy as jnp
import numpy as np
from jax import lax

DET = 3
BINS = 128
FINE = 8192
MOST_FINE = 128
TSHIFT = 2048
DRAWS = 32768


def draw_proposal_log(key, part):
    values = jax.random.normal(jax.random.fold_in(key, 72), (DRAWS,), jnp.float32)
    return jnp.clip(values, -3.0, 3.0)


def levels(key, extent, cuts, smallest, high):
    level, own = 1.0, jax.random.fold_in(key, 6)
    for dim, blocks in cuts:
        draws = jnp.exp(jax.random.uniform(jax.random.fold_in(own, dim), (blocks,), jnp.float32, smallest / len(cuts), high / len(cuts)))
        level = level * jnp.repeat(draws, extent[dim] // blocks).reshape([-1 if axis == dim else 1 for axis in range(len(extent))])
    return level


def profile(count, total, bound, skew):
    loads = [(1 << 20) // math.isqrt(standing ** skew) + 1 for standing in range(2, count + 1)]
    rest, given = total - bound - (count - 1), [1] * (count - 1)
    while rest > 0:
        free = [i for i in range(count - 1) if given[i] < bound]
        mass, budget = sum([loads[i] for i in free]), rest
        for i in free:
            extra = min(bound - given[i], max(1, budget * loads[i] // mass), rest)
            given[i] = given[i] + extra
            rest = rest - extra
    return np.array([bound] + given)


def ragged(stream_key, amount, total, reach, lean):
    if amount == 2:
        one = jax.random.randint(stream_key, (), max(1, total - reach), min(reach, total - 1) + 1)
        return jnp.stack([one, total - one])
    lengths = jnp.asarray(profile(amount, total, reach, lean), jnp.int32)
    pairs = (amount - 1) // 2
    giver, sink = lengths[1:1 + 2 * pairs:2], lengths[2:2 + 2 * pairs:2]
    room = jnp.minimum(giver - 1, reach - sink)
    shifted = jax.random.randint(jax.random.fold_in(stream_key, 1), (pairs,), 0, 1 << 20) % (room + 1)
    lengths = lengths.at[1:1 + 2 * pairs:2].set(giver - shifted).at[2:2 + 2 * pairs:2].set(sink + shifted)
    return lengths[jax.random.permutation(jax.random.fold_in(stream_key, 2), amount)]


def noise(key, dims, width, limit, cuts=(), kind=jnp.bfloat16):
    drawn = jax.random.normal(key, dims, jnp.float32) * width
    if len(cuts) > 0:
        drawn = levels(key, dims, cuts, -0.22, 0.18) * drawn
    return jnp.clip(drawn, min=-limit, max=limit).astype(kind)


def setup_inputs(seed: int = 0, part: int = 0) -> dict:
    arg_keys = jax.random.split(jax.random.key(seed), 9)
    part_keys = jax.random.split(jax.random.fold_in(arg_keys[8], part), 9)
    return {
        "fine_cross": noise(part_keys[0], (DET, 2, FINE), 0.025, 0.15, ((2, 32),), jnp.float32),
        "fine_power": jnp.clip(jnp.exp(math.log(0.005) - 3.6888794 * jax.random.uniform(part_keys[1], (DET, FINE), jnp.float32) ** levels(part_keys[1], (DET, FINE), ((1, 32),), -0.2, 0.2)), 0.000125, 0.005),
        "bin_widths": ragged(part_keys[2], BINS, FINE, MOST_FINE, 1).astype(jnp.int32),
        "log_amps": noise(part_keys[3], (DET, DRAWS), 0.1, 0.5, ((1, 32),), jnp.float32),
        "delays": noise(part_keys[4], (DET, DRAWS), 0.3, 1.5, ((1, 32),), jnp.float32),
        "phases": jnp.clip(jax.random.uniform(part_keys[5], (DRAWS,), jnp.float32, -3.140625, 3.140625), -3.140625, 3.140625),
        "chirps": noise(part_keys[6], (DRAWS,), 2.0, 8.0, ((0, 32),), jnp.float32),
        "proposal_log": draw_proposal_log(jax.random.fold_in(jax.random.fold_in(arg_keys[8], part), 71), part),
    }


TWO_PI = 2.0 * math.pi
TIME_STEP = 0.125
PRECISE = lax.Precision.HIGHEST


def summary_terms(cross_rows, power_rows, first_fine, lower_edge, bin_widths):
    fine_index = first_fine + jnp.arange(power_rows.shape[1], dtype=jnp.int32)
    upper_edge = lower_edge + bin_widths
    inside = ((fine_index[:, None] >= lower_edge[None, :]) & (fine_index[:, None] < upper_edge[None, :])).astype(jnp.float32)
    offset = fine_index.astype(jnp.float32)[:, None] + 0.5 - lower_edge.astype(jnp.float32)[None, :]
    weight = inside * offset / bin_widths.astype(jnp.float32)[None, :]
    lower_weight = inside - weight
    detectors = power_rows.shape[0]
    flattened = cross_rows.reshape(detectors * 2, -1)
    start_sums = jnp.dot(flattened, lower_weight, precision=PRECISE).reshape(detectors, 2, -1)
    end_sums = jnp.dot(flattened, weight, precision=PRECISE).reshape(detectors, 2, -1)
    power_low = jnp.dot(power_rows, lower_weight * lower_weight, precision=PRECISE)
    power_mixed = jnp.dot(power_rows, lower_weight * weight, precision=PRECISE)
    power_high = jnp.dot(power_rows, weight * weight, precision=PRECISE)
    return start_sums, end_sums, power_low, power_mixed, power_high


def edge_phase(freq_values, delays, phases, chirps):
    return ((TWO_PI * freq_values)[None, :, None] * delays[:, None, :] + phases[None, None, :]
            + chirps[None, None, :] * (freq_values * freq_values)[None, :, None])


def sample_terms(freq_low, freq_high, log_amps, delays, phases, chirps, power_low, power_mixed, power_high):
    amplitude = jnp.exp(log_amps)[:, None, :]
    phase_low = edge_phase(freq_low, delays, phases, chirps)
    phase_high = edge_phase(freq_high, delays, phases, chirps)
    pair_low = jnp.stack([amplitude * jnp.cos(phase_low), amplitude * jnp.sin(phase_low)], axis=2)
    pair_high = jnp.stack([amplitude * jnp.cos(phase_high), amplitude * jnp.sin(phase_high)], axis=2)
    features = jnp.stack([pair_low, pair_high], axis=2).reshape(-1, log_amps.shape[1])
    cos_diff = jnp.cos(phase_low - phase_high)
    inner_sum = jnp.sum(power_low + power_high, axis=1)[:, None] + 2.0 * jnp.einsum(
        'db,dbn->dn', power_mixed, cos_diff, precision=PRECISE)
    self_power = jnp.sum(jnp.exp(2.0 * log_amps) * inner_sum, axis=0)
    return features, self_power


def build_table(first_shift, row_count, total_shifts, start_sums, end_sums, freq_low, freq_high):
    shifts = (first_shift + jnp.arange(row_count, dtype=jnp.int32) - total_shifts // 2).astype(jnp.float32) * TIME_STEP
    edge_freq = jnp.stack([freq_low, freq_high], axis=-1)
    angles = (TWO_PI * edge_freq)[None] * shifts[:, None, None]
    cosine = jnp.cos(angles)[:, None]
    sine_value = jnp.sin(angles)[:, None]
    real_part = jnp.stack([start_sums[:, 0], end_sums[:, 0]], axis=-1)[None]
    imag_part = jnp.stack([start_sums[:, 1], end_sums[:, 1]], axis=-1)[None]
    table_real = real_part * cosine + imag_part * sine_value
    table_imag = imag_part * cosine - real_part * sine_value
    return jnp.stack([table_real, table_imag], axis=-1).reshape(row_count, -1)


def reference(fine_cross, fine_power, bin_widths, log_amps, delays, phases, chirps, proposal_log):
    upper_edge = jnp.cumsum(bin_widths).astype(jnp.int32)
    lower_edge = (upper_edge - bin_widths).astype(jnp.int32)
    start_sums, end_sums, power_low, power_mixed, power_high = summary_terms(
        fine_cross, fine_power, jnp.int32(0), lower_edge, bin_widths)
    freq_low = lower_edge.astype(jnp.float32) / FINE
    freq_high = upper_edge.astype(jnp.float32) / FINE
    features, self_power = sample_terms(freq_low, freq_high, log_amps, delays, phases, chirps,
                                        power_low, power_mixed, power_high)
    matrix = build_table(jnp.int32(0), TSHIFT, TSHIFT, start_sums, end_sums, freq_low, freq_high)
    cross_terms = jnp.dot(matrix, features, precision=PRECISE)
    scores = cross_terms - 0.5 * self_power[None, :] + proposal_log[None, :]
    largest = jnp.max(scores, axis=0)
    marginal = largest + jnp.log(jnp.sum(jnp.exp(scores - largest[None, :]), axis=0)) - math.log(TSHIFT)
    peak_value = jnp.max(marginal)
    total_log = peak_value + jnp.log(jnp.sum(jnp.exp(marginal - peak_value)))
    return marginal - total_log, (total_log - math.log(DRAWS)).reshape(1)
```

```python
import math

import jax
import jax.numpy as jnp
import numpy as np
from jax import lax
from jax.experimental import pallas as pl
from jax.experimental.pallas import tpu as pltpu
from jax.sharding import PartitionSpec as P

TSHIFT = 2048
TIME_STEP = 0.125
CHUNK = 256
LANES = 128
ROWS = 5
VMEM = pl.BlockSpec(memory_space=pltpu.VMEM)
F32, BF16 = jnp.float32, jnp.bfloat16


def fit(function, terms):
    nodes = 0.125 * (1.0 + np.cos((np.arange(64) + 0.5) * np.pi / 64))
    basis = np.vander(nodes / 0.25, terms, increasing=True)
    found = np.linalg.lstsq(basis, function(np.sqrt(nodes)), rcond=None)[0]
    return [float(c) for c in found / 0.25 ** np.arange(terms)]


COS = fit(lambda r: np.cos(2 * np.pi * r), 9)
SIN = fit(lambda r: np.sin(2 * np.pi * r) / r, 9)


def horner(coefficients, x):
    total = jnp.full_like(x, coefficients[-1])
    for c in coefficients[-2::-1]:
        total = total * x + c
    return total


def turn(u):
    r = u - jnp.round(u)
    square = r * r
    return horner(COS, square), horner(SIN, square) * r


def call(kernel, outs, *args, limit=24 << 20, flops=1 << 20, name=None):
    return pl.pallas_call(
        kernel,
        out_shape=outs,
        in_specs=[VMEM] * len(args),
        out_specs=jax.tree.map(lambda _: VMEM, outs),
        compiler_params=pltpu.CompilerParams(vmem_limit_bytes=limit),
        cost_estimate=pl.CostEstimate(flops=flops, bytes_accessed=1 << 20, transcendentals=0),
        name=name,
    )(*args)


def edges(widths):
    wide = widths.astype(F32)
    bins = wide.shape[1]
    before = lax.broadcasted_iota(jnp.int32, (bins, bins), 0)
    mine = lax.broadcasted_iota(jnp.int32, (bins, bins), 1)
    ones = jnp.where(before <= mine, 1.0, 0.0).astype(BF16)
    rows = jnp.broadcast_to(wide, (16, bins)).astype(BF16)
    upper = jnp.dot(rows, ones, preferred_element_type=F32)[:1]
    return wide, upper


def split(x):
    high = x.astype(BF16)
    return high, (x - high.astype(F32)).astype(BF16)


def summary_kernel(cross_ref, power_ref, widths_ref, out_ref):
    fine, bins = power_ref.shape[1], widths_ref.shape[1]
    wide, upper = edges(widths_ref[...])
    lower = upper - wide
    first = (lax.axis_index("draw") * fine).astype(F32)
    at = lax.broadcasted_iota(jnp.int32, (fine, bins), 0).astype(F32) + first
    inside = (at >= lower) & (at < upper)
    up = jnp.where(inside, 2.0 * (at - lower) + 1.0, 0.0)
    down = jnp.where(inside, 2.0 * wide - up, 0.0)
    both_high, both_low = split(up * down)
    weights = jnp.concatenate([up.astype(BF16), down.astype(BF16), both_high, both_low], axis=1)
    data = jnp.concatenate(
        [cross_ref[...], power_ref[...], jnp.zeros((7, fine), F32)], axis=0
    )
    high = data.astype(BF16)
    rest = data - high.astype(F32)
    middle, low = split(rest)
    got = jnp.dot(
        jnp.concatenate([high, middle, low], axis=0), weights, preferred_element_type=F32
    )
    got = got[:16] + got[16:32] + got[32:]
    scale = 0.5 / wide
    end = got[:, :bins] * scale
    start = got[:, bins : 2 * bins] * scale
    mixed = (got[:, 2 * bins : 3 * bins] + got[:, 3 * bins :]) * (scale * scale)
    row = lax.broadcasted_iota(jnp.int32, (16, bins), 0)
    lane = lax.broadcasted_iota(jnp.int32, (16, bins), 1)
    merged = end + jnp.where(lane < bins - 1, pltpu.roll(start, bins - 1, 1), 0.0)
    total = jnp.sum(data, axis=1, keepdims=True)
    single = jnp.where(row < 6, start[:, :1], total)
    single = jnp.sum(jnp.where(lane == row, single, 0.0), axis=0, keepdims=True)
    table = jnp.where(row < 6, merged, mixed)
    table = jnp.where(row == 9, single, table)
    mine = lax.axis_index("bin")
    for r in range(ROWS):
        line = jnp.where(mine == 0, table[r : r + 1], table[ROWS + r : ROWS + r + 1])
        out_ref[:, :, r * bins : (r + 1) * bins] = jnp.broadcast_to(
            line[None], (out_ref.shape[0], 1, bins)
        )


def terms_kernel(
    widths_ref, amps_ref, delays_ref, phases_ref, chirps_ref, prior_ref,
    high_ref, low_ref, features_ref, spread_ref, flat_ref, grid=0.0,
):
    wide, upper = edges(widths_ref[...])
    bins = wide.shape[1]
    draws = features_ref.shape[2]
    mine = pl.ds(pl.multiple_of(lax.axis_index("bin") * draws, draws), draws)
    for c in range(TSHIFT // CHUNK):
        shift = lax.broadcasted_iota(jnp.int32, (CHUNK, bins), 0).astype(F32)
        shift = shift + float(c * CHUNK - TSHIFT // 2)
        cosine, sine = turn((shift * upper) * (TIME_STEP / grid))
        rows = slice(c * CHUNK, (c + 1) * CHUNK)
        high_ref[rows, :bins], low_ref[rows, :bins] = split(cosine)
        high_ref[rows, bins:], low_ref[rows, bins:] = split(sine)
    tall = jnp.concatenate(
        [wide, upper, jnp.zeros((bins - 2, bins), F32)], axis=0
    ).T
    width, x = tall[:, :1] * (1.0 / grid), tall[:, 1:2] * (1.0 / grid)
    phases, chirps = phases_ref[:, mine], chirps_ref[:, mine]
    base = phases * (0.5 / math.pi)
    bend = chirps * (0.5 / math.pi)
    common = base + bend * (x * x)
    half_bend = (0.5 * width * (x + (x - width))) * chirps
    cos0, sin0 = turn(base)
    for d in range(3):
        amp = jnp.exp(amps_ref[d : d + 1, mine])
        delay = delays_ref[d : d + 1, mine]
        cosine, sine = turn(x * delay + common)
        features_ref[2 * d] = amp * cosine
        features_ref[2 * d + 1] = amp * sine
        half = (math.pi * width) * delay + half_bend
        h2 = half * half
        sh = half * (1.0 + h2 * (-1.0 / 6 + h2 * (1.0 / 120 + h2 * (-1.0 / 5040))))
        spread_ref[d] = (2.0 * amp * sh) * (amp * sh)
        flat_ref[2 * d : 2 * d + 1] = amp * cos0
        flat_ref[2 * d + 1 : 2 * d + 2] = amp * sin0
        flat_ref[6 + d : 7 + d] = (-0.5 * amp) * amp
    flat_ref[9:10] = prior_ref[:, mine]


def score_kernel(sums_ref, high_ref, low_ref, features_ref, spread_ref, flat_ref, out_ref, stat_ref):
    bins = features_ref.shape[1]
    draws = features_ref.shape[2]
    lines = [
        sums_ref[r // ROWS, :, (r % ROWS) * bins : (r % ROWS + 1) * bins] for r in range(2 * ROWS)
    ]
    single = lines[9]
    tall = jnp.concatenate(lines[:9] + [jnp.zeros((bins - 9, bins), F32)], axis=0).T
    real = imag = power = None
    offset = flat_ref[9:10]
    for d in range(3):
        a, b, mixed = tall[:, 2 * d : 2 * d + 1], tall[:, 2 * d + 1 : 2 * d + 2], tall[:, 6 + d : 7 + d]
        cosine, sine = features_ref[2 * d], features_ref[2 * d + 1]
        re, im, pw = a * cosine + b * sine, b * cosine - a * sine, mixed * spread_ref[d]
        real = re if real is None else real + re
        imag = im if imag is None else imag + im
        power = pw if power is None else power + pw
        offset = (
            offset
            + single[:, 2 * d : 2 * d + 1] * flat_ref[2 * d : 2 * d + 1]
            + single[:, 2 * d + 1 : 2 * d + 2] * flat_ref[2 * d + 1 : 2 * d + 2]
            + single[:, 6 + d : 7 + d] * flat_ref[6 + d : 7 + d]
        )
    offset = offset + jnp.sum(power, axis=0, keepdims=True)
    wide_high, wide_low = split(jnp.concatenate([real, imag], axis=0))
    top = total = None
    for c in range(TSHIFT // CHUNK):
        rows = slice(c * CHUNK, (c + 1) * CHUNK)
        high, low = high_ref[rows, :], low_ref[rows, :]
        cross = (
            jnp.dot(high, wide_high, preferred_element_type=F32)
            + jnp.dot(high, wide_low, preferred_element_type=F32)
            + jnp.dot(low, wide_high, preferred_element_type=F32)
        )
        cross = cross.reshape(CHUNK // 8, 8, draws)
        peak = jnp.max(cross, axis=0)
        if top is not None:
            peak = jnp.maximum(peak, top)
            total = total * jnp.exp(top - peak)
        add = jnp.sum(jnp.exp(cross - peak[None]), axis=0)
        total = add if total is None else total + add
        top = peak
    peak = jnp.max(top, axis=0, keepdims=True)
    total = jnp.sum(total * jnp.exp(top - peak), axis=0, keepdims=True)
    marginal = (peak + jnp.log(total) - math.log(TSHIFT)) + offset
    out_ref[...] = marginal
    best = jnp.max(marginal, axis=1, keepdims=True)
    mass = jnp.sum(jnp.exp(marginal - best), axis=1, keepdims=True)
    lane = lax.broadcasted_iota(jnp.int32, (1, LANES), 1)
    stat = jnp.where(lane == 0, best, mass)
    stat_ref[...] = jnp.broadcast_to(stat[None], stat_ref.shape)


def final_kernel(stats_ref, marginal_ref, out_ref, evidence_ref, draws=0):
    stats = stats_ref[...]
    best, mass = stats[:, :, :1], stats[:, :, 1:2]
    top = jnp.max(best, axis=0, keepdims=True)
    total = top + jnp.log(jnp.sum(mass * jnp.exp(best - top), axis=0, keepdims=True))
    out_ref[...] = marginal_ref[...] - total
    evidence_ref[...] = total[0] - math.log(draws)


def body(fine_cross, fine_power, bin_widths, log_amps, delays, phases, chirps, proposal_log):
    shards, cores = lax.axis_size("draw"), lax.axis_size("bin")
    detectors, fine = fine_power.shape
    bins = bin_widths.shape[0]
    whole = log_amps.shape[1]
    draws = whole // cores
    widths = bin_widths.reshape(1, bins)
    sums = call(
        summary_kernel,
        jax.ShapeDtypeStruct((shards, 1, ROWS * bins), F32),
        fine_cross.reshape(2 * detectors, fine), fine_power, widths,
        flops=1 << 24, name="summary",
    )
    everyone = lax.all_to_all(sums, "draw", 0, 0, tiled=True)
    high, low, features, spread, flat = call(
        lambda *refs: terms_kernel(*refs, grid=float(fine * shards)),
        (
            jax.ShapeDtypeStruct((TSHIFT, 2 * bins), BF16),
            jax.ShapeDtypeStruct((TSHIFT, 2 * bins), BF16),
            jax.ShapeDtypeStruct((2 * detectors, bins, draws), F32),
            jax.ShapeDtypeStruct((detectors, bins, draws), F32),
            jax.ShapeDtypeStruct((16, draws), F32),
        ),
        widths, log_amps, delays, phases.reshape(1, whole), chirps.reshape(1, whole),
        proposal_log.reshape(1, whole), flops=1 << 28, name="terms",
    )
    added = jnp.sum(everyone, axis=0, keepdims=True)
    joined = lax.all_gather(added, "bin", axis=0, tiled=True)
    marginal, stat = call(
        score_kernel,
        (
            jax.ShapeDtypeStruct((1, draws), F32),
            jax.ShapeDtypeStruct((shards * cores, 1, LANES), F32),
        ),
        joined, high, low, features, spread, flat, flops=1 << 30, name="score",
    )
    stats = lax.all_to_all(stat, ("draw", "bin"), 0, 0, tiled=True)
    marginals = lax.all_gather(marginal.reshape(1, 1, draws), "bin", axis=0, tiled=True)
    weights, evidence = call(
        lambda *refs: final_kernel(*refs, draws=whole * shards),
        (
            jax.ShapeDtypeStruct((cores, 1, draws), F32),
            jax.ShapeDtypeStruct((1, 1), F32),
        ),
        stats, marginals, name="final",
    )
    return weights.reshape(whole), evidence.reshape(1)


def solution(mesh):
    placed = (
        P("event", None, "draw"),
        P("event", "draw"),
        P("event"),
        P("event", "draw"),
        P("event", "draw"),
        P(("event", "draw")),
        P(("event", "draw")),
        P(("event", "draw")),
    )
    return jax.shard_map(
        body,
        mesh=mesh,
        in_specs=placed,
        out_specs=(P(("event", "draw")), P("event")),
        check_vma=False,
    )
```

```python
import functools
import math

import jax
import jax.numpy as jnp
import numpy as np
from jax import lax
from jax.experimental import pallas as pl
from jax.experimental.pallas import tpu as pltpu
from jax.sharding import PartitionSpec as P

TSHIFT = 2048
TIME_STEP = 0.125
CHUNK = 128
TAIL = 16
LANES = 128
DET = 3
CHANNELS = 9
SPAN = 71
ROWS = 5
MEET = 0.75
VMEM = pl.BlockSpec(memory_space=pltpu.VMEM)
F32, BF16 = jnp.float32, jnp.bfloat16


def fit(function, terms):
    nodes = 0.125 * (1.0 + np.cos((np.arange(64) + 0.5) * np.pi / 64))
    basis = np.vander(nodes / 0.25, terms, increasing=True)
    found = np.linalg.lstsq(basis, function(np.sqrt(nodes)), rcond=None)[0]
    return [float(c) for c in found / 0.25 ** np.arange(terms)]


COS = fit(lambda r: np.cos(np.pi * r), 7)
SIN = fit(lambda r: np.sin(np.pi * r) / r, 6)


def horner(coefficients, x):
    total = jnp.full_like(x, coefficients[-1])
    for c in coefficients[-2::-1]:
        total = total * x + c
    return total


def turn(u):
    r = u - jnp.round(u)
    square = r * r
    cosine, sine = horner(COS, square), horner(SIN, square) * r
    twice = sine + sine
    return 1.0 - twice * sine, twice * cosine


def call(kernel, outs, *args, scratch=None, limit=24 << 20, flops=1 << 20, name=None):
    where = VMEM
    if scratch is not None:
        where = pl.BlockSpec(memory_space=pltpu.HBM)
        args = [pltpu.with_memory_space_constraint(a, pltpu.HBM) for a in args]
    return pl.pallas_call(
        kernel,
        out_shape=outs,
        in_specs=[where] * len(args),
        out_specs=jax.tree.map(lambda _: VMEM, outs),
        scratch_shapes=() if scratch is None else scratch,
        compiler_params=pltpu.CompilerParams(vmem_limit_bytes=limit),
        cost_estimate=pl.CostEstimate(flops=flops, bytes_accessed=1 << 20, transcendentals=0),
        name=name,
    )(*args)


def landing(args):
    return [pltpu.VMEM(a.shape, a.dtype) for a in args] + [pltpu.SemaphoreType.DMA((len(args),))]


def fetch(sources, targets, semaphores):
    copies = [
        pltpu.make_async_copy(source, target, semaphores.at[i])
        for i, (source, target) in enumerate(zip(sources, targets))
    ]
    for copy in copies:
        copy.start()
    return copies


def shifted(x, amount):
    for bit in range(LANES.bit_length() - 1):
        x = jnp.where((amount >> bit) & 1 == 1, pltpu.roll(x, 1 << bit, 1), x)
    return x


def edges(widths):
    wide = widths.astype(F32)
    bins = wide.shape[1]
    before = lax.broadcasted_iota(jnp.int32, (bins, bins), 0)
    mine = lax.broadcasted_iota(jnp.int32, (bins, bins), 1)
    ones = jnp.where(before <= mine, 1.0, 0.0).astype(BF16)
    rows = jnp.broadcast_to(wide, (16, bins)).astype(BF16)
    upper = jnp.dot(rows, ones, preferred_element_type=F32)[:1]
    return wide, upper


def split(x):
    high = x.astype(BF16)
    return high, (x - high.astype(F32)).astype(BF16)


def summary_kernel(cross_in, power_in, widths_in, out_ref, cross_ref, power_ref, widths_ref, sems):
    for copy in fetch(
        (widths_in, cross_in, power_in), (widths_ref, cross_ref, power_ref), sems
    ):
        copy.wait()
    fine, bins = power_ref.shape[1], widths_ref.shape[1]
    wide, upper = edges(widths_ref[...])
    lower = upper - wide
    first = (lax.axis_index("draw") * fine).astype(F32)
    at = lax.broadcasted_iota(jnp.int32, (fine, bins), 0).astype(F32) + first
    inside = (at >= lower) & (at < upper)
    up = jnp.where(inside, 2.0 * (at - lower) + 1.0, 0.0)
    down = jnp.where(inside, 2.0 * wide - up, 0.0)
    both_high, both_low = split(up * down)
    weights = jnp.concatenate([up.astype(BF16), down.astype(BF16), both_high, both_low], axis=1)
    data = jnp.concatenate(
        [cross_ref[d] for d in range(DET)] + [power_ref[...], jnp.zeros((7, fine), F32)], axis=0
    )
    high = data.astype(BF16)
    rest = data - high.astype(F32)
    middle, low = split(rest)
    got = jnp.dot(
        jnp.concatenate([high, middle, low], axis=0), weights, preferred_element_type=F32
    )
    got = got[:16] + got[16:32] + got[32:]
    scale = 0.5 / wide
    end = got[:, :bins] * scale
    start = got[:, bins : 2 * bins] * scale
    mixed = (got[:, 2 * bins : 3 * bins] + got[:, 3 * bins :]) * (scale * scale)
    row = lax.broadcasted_iota(jnp.int32, (16, bins), 0)
    lane = lax.broadcasted_iota(jnp.int32, (16, bins), 1)
    merged = end + pltpu.roll(start, bins - 1, 1)
    passed = jnp.sum(jnp.where(upper <= first, 1, 0), axis=1, keepdims=True)
    table = shifted(jnp.where(row < 6, merged, mixed), (bins + 1 - passed) % bins)
    total = jnp.sum(data, axis=1, keepdims=True)
    table = jnp.where((row >= 6) & (lane == SPAN - 1), total, table)
    lane = lane[:1]
    tiles = [jnp.zeros((1, bins), F32)] * (ROWS + 1)
    for c in range(CHANNELS):
        tile, off = divmod(c * SPAN, bins)
        line = pltpu.roll(table[c : c + 1], off, 1) if off else table[c : c + 1]
        tiles[tile] = tiles[tile] + jnp.where(lane >= off, line, 0.0)
        tiles[tile + 1] = tiles[tile + 1] + jnp.where(lane < off, line, 0.0)
    for r in range(ROWS):
        out_ref[:, :, r * bins : (r + 1) * bins] = jnp.broadcast_to(
            tiles[r][None], (out_ref.shape[0], 1, bins)
        )


def terms_kernel(
    widths_in, amps_in, delays_in, phases_in, chirps_in, prior_in,
    cos_ref, sin_ref, features_ref, spread_ref, flat_ref, place_ref,
    widths_ref, amps_ref, delays_ref, phases_ref, chirps_ref, prior_ref, sems,
    grid=0.0, fine=0, start=0,
):
    copies = fetch(
        (widths_in, amps_in, delays_in, phases_in, chirps_in, prior_in),
        (widths_ref, amps_ref, delays_ref, phases_ref, chirps_ref, prior_ref),
        sems,
    )
    copies[0].wait()
    wide, upper = edges(widths_ref[...])
    bins = wide.shape[1]
    draws = features_ref.shape[2]
    mine = pl.ds(pl.multiple_of(lax.axis_index("bin") * draws, draws), draws)
    member = lax.broadcasted_iota(jnp.int32, place_ref.shape, 0)
    source = (member + start) % place_ref.shape[0] * fine
    passed = jnp.sum(jnp.where(upper <= source.astype(F32), 1, 0), axis=1, keepdims=True)
    place_ref[...] = jnp.broadcast_to((passed + (bins - 1)) % bins, place_ref.shape)
    step = upper * (TIME_STEP / grid)
    near = lax.broadcasted_iota(jnp.int32, (CHUNK, bins), 0).astype(F32)
    near_cos, near_sin = turn(near * step)
    for first in range(0, TSHIFT // 2 + TAIL, CHUNK):
        size = min(CHUNK, TSHIFT // 2 + TAIL - first)
        rows = slice(first, first + size)
        far_cos, far_sin = turn(float(first) * step)
        here_cos, here_sin = near_cos[:size], near_sin[:size]
        cosine = here_cos * far_cos - here_sin * far_sin
        sine = here_sin * far_cos + here_cos * far_sin
        cos_ref[rows, :bins], cos_ref[rows, bins:] = split(cosine)
        sin_ref[rows, :bins], sin_ref[rows, bins:] = split(sine)
    tall = jnp.concatenate([wide, upper, jnp.zeros((bins - 2, bins), F32)], axis=0).T
    width, x = tall[:, :1] * (1.0 / grid), tall[:, 1:2] * (1.0 / grid)
    for copy in copies[1:]:
        copy.wait()
    chirps = chirps_ref[:, mine]
    base = phases_ref[:, mine] * (0.5 / math.pi)
    common = base + (chirps * (0.5 / math.pi)) * (x * x)
    half_bend = (0.5 * width * (x + (x - width))) * chirps
    cos0, sin0 = turn(base)
    for d in range(DET):
        amp = jnp.exp(amps_ref[d : d + 1, mine])
        delay = delays_ref[d : d + 1, mine]
        cosine, sine = turn(x * delay + common)
        features_ref[2 * d] = amp * cosine
        features_ref[2 * d + 1] = amp * sine
        half = (math.pi * width) * delay + half_bend
        h2 = half * half
        sh = half * (1.0 + h2 * (-1.0 / 6 + h2 * (1.0 / 120 + h2 * (-1.0 / 5040))))
        spread_ref[d] = (2.0 * amp * sh) * (amp * sh)
        flat_ref[2 * d : 2 * d + 1] = amp * cos0
        flat_ref[2 * d + 1 : 2 * d + 2] = amp * sin0
    flat_ref[6:7] = prior_ref[:, mine]


def score_kernel(
    sums_ref, cos_ref, sin_ref, features_ref, spread_ref, flat_ref, place_ref, out_ref, stat_ref,
    zero=0,
):
    bins = features_ref.shape[1]
    draws = features_ref.shape[2]
    place = place_ref[...]
    row = lax.broadcasted_iota(jnp.int32, place.shape, 0)
    lane = lax.broadcasted_iota(jnp.int32, place.shape, 1)
    tiles = [sums_ref[:, 0, r * bins : (r + 1) * bins] for r in range(ROWS)] + [None]
    lines, single = [], []
    for c in range(CHANNELS):
        tile, off = divmod(c * SPAN, bins)
        line = pltpu.roll(tiles[tile], bins - off, 1) if off else tiles[tile]
        if off + SPAN > bins:
            line = jnp.where(lane < bins - off, line, pltpu.roll(tiles[tile + 1], bins - off, 1))
        if c >= 6:
            at_end = jnp.sum(line, axis=0, keepdims=True)[:, SPAN - 1 : SPAN]
        line = shifted(jnp.where(lane < SPAN - (1 if c >= 6 else 0), line, 0.0), place)
        if c < 6:
            at_end = line[zero : zero + 1, bins - 1 :]
            line = jnp.where((row == zero) & (lane == bins - 1), 0.0, line)
        single.append(at_end)
        lines.append(jnp.sum(line, axis=0, keepdims=True))
    tall = jnp.concatenate(lines + [jnp.zeros((bins - CHANNELS, bins), F32)], axis=0).T
    real = imag = power = None
    offset = flat_ref[6:7]
    for d in range(DET):
        a, b, mixed = tall[:, 2 * d : 2 * d + 1], tall[:, 2 * d + 1 : 2 * d + 2], tall[:, 6 + d : 7 + d]
        cosine, sine = features_ref[2 * d], features_ref[2 * d + 1]
        re, im, pw = a * cosine + b * sine, b * cosine - a * sine, mixed * spread_ref[d]
        real = re if real is None else real + re
        imag = im if imag is None else imag + im
        power = pw if power is None else power + pw
        cos0, sin0 = flat_ref[2 * d : 2 * d + 1], flat_ref[2 * d + 1 : 2 * d + 2]
        offset = offset + single[2 * d] * cos0 + single[2 * d + 1] * sin0
        offset = offset - (0.5 * single[6 + d]) * (cos0 * cos0 + sin0 * sin0)
    offset = offset + jnp.sum(power, axis=0, keepdims=True)
    real, imag = (
        [jnp.concatenate([half, half], axis=0) for half in split(part)] for part in (real, imag)
    )

    def rotated(rows):
        return (
            jnp.dot(ref[rows, :], part[0], preferred_element_type=F32)
            + jnp.dot(ref[rows, :], part[1], preferred_element_type=F32)
            for ref, part in ((cos_ref, real), (sin_ref, imag))
        )

    even, odd = rotated(slice(TSHIFT // 2, TSHIFT // 2 + TAIL))
    earliest = (even - odd)[:1]
    top = total = None
    for first in range(0, TSHIFT // 2, CHUNK):
        even, odd = rotated(slice(first, first + CHUNK))
        after, before = even + odd, even - odd
        if first == 0:
            at = lax.broadcasted_iota(jnp.int32, before.shape, 0)
            before = jnp.where(at == 0, earliest, before)
        after = after.reshape(CHUNK // 8, 8, draws)
        before = before.reshape(CHUNK // 8, 8, draws)
        peak = jnp.max(jnp.maximum(after, before), axis=0)
        if top is not None:
            peak = jnp.maximum(peak, top)
            total = total * jnp.exp(top - peak)
        add = jnp.sum(jnp.exp(after - peak[None]) + jnp.exp(before - peak[None]), axis=0)
        total = add if total is None else total + add
        top = peak
    peak = jnp.max(top, axis=0, keepdims=True)
    total = jnp.sum(total * jnp.exp(top - peak), axis=0, keepdims=True)
    marginal = (peak + jnp.log(total) - math.log(TSHIFT)) + offset
    out_ref[...] = marginal
    best = jnp.max(marginal, axis=1, keepdims=True)
    mass = jnp.sum(jnp.exp(marginal - best), axis=1, keepdims=True)
    lane = lax.broadcasted_iota(jnp.int32, (1, LANES), 1)
    stat = jnp.where(lane == 0, best, mass)
    stat_ref[...] = jnp.broadcast_to(stat[None], stat_ref.shape)


def final_kernel(stats_ref, marginal_ref, out_ref, evidence_ref, draws=0):
    stats = stats_ref[...]
    best, mass = stats[:, :, :1], stats[:, :, 1:2]
    top = jnp.max(best, axis=0, keepdims=True)
    total = top + jnp.log(jnp.sum(mass * jnp.exp(best - top), axis=0, keepdims=True))
    out_ref[...] = marginal_ref[...] - total
    evidence_ref[...] = total[0] - math.log(draws)


def body(fine_cross, fine_power, bin_widths, log_amps, delays, phases, chirps, proposal_log):
    shards, cores = lax.axis_size("draw"), lax.axis_size("bin")
    detectors, fine = fine_power.shape
    bins = bin_widths.shape[0]
    whole = log_amps.shape[1]
    draws = whole // cores
    widths = bin_widths.reshape(1, bins)
    turned = [(i + int(shards * MEET)) % shards for i in range(shards)]
    args = (fine_cross, fine_power, widths)
    sums = call(
        summary_kernel,
        jax.ShapeDtypeStruct((shards, 1, ROWS * bins), F32),
        *args, scratch=landing(args), flops=1 << 24, name="summary",
    )
    everyone = lax.all_to_all(sums, "draw", 0, 0, axis_index_groups=[turned], tiled=True)
    args = (
        widths, log_amps, delays, phases.reshape(1, whole), chirps.reshape(1, whole),
        proposal_log.reshape(1, whole),
    )
    terms = call(
        functools.partial(terms_kernel, grid=float(fine * shards), fine=fine, start=turned[0]),
        (
            jax.ShapeDtypeStruct((TSHIFT // 2 + TAIL, 2 * bins), BF16),
            jax.ShapeDtypeStruct((TSHIFT // 2 + TAIL, 2 * bins), BF16),
            jax.ShapeDtypeStruct((2 * detectors, bins, draws), F32),
            jax.ShapeDtypeStruct((detectors, bins, draws), F32),
            jax.ShapeDtypeStruct((8, draws), F32),
            jax.ShapeDtypeStruct((shards, bins), jnp.int32),
        ),
        *args, scratch=landing(args), flops=1 << 28, name="terms",
    )
    marginal, stat = call(
        functools.partial(score_kernel, zero=turned.index(0)),
        (
            jax.ShapeDtypeStruct((1, draws), F32),
            jax.ShapeDtypeStruct((shards * cores, 1, LANES), F32),
        ),
        everyone, *terms, flops=1 << 30, name="score",
    )
    both = [i * cores + c for i in turned for c in range(cores)]
    stats = lax.all_to_all(
        stat, ("draw", "bin"), 0, 0, axis_index_groups=[both], tiled=True
    )
    marginals = lax.all_gather(marginal.reshape(1, 1, draws), "bin", axis=0, tiled=True)
    weights, evidence = call(
        lambda *refs: final_kernel(*refs, draws=whole * shards),
        (
            jax.ShapeDtypeStruct((cores, 1, draws), F32),
            jax.ShapeDtypeStruct((1, 1), F32),
        ),
        stats, marginals, name="final",
    )
    return weights.reshape(whole), evidence.reshape(1)


def solution(mesh):
    placed = (
        P("event", None, "draw"),
        P("event", "draw"),
        P("event"),
        P("event", "draw"),
        P("event", "draw"),
        P(("event", "draw")),
        P(("event", "draw")),
        P(("event", "draw")),
    )
    return jax.shard_map(
        body,
        mesh=mesh,
        in_specs=placed,
        out_specs=(P(("event", "draw")), P("event")),
        check_vma=False,
    )
```

```python
import functools
import math

import jax
import jax.numpy as jnp
import numpy as np
from jax import lax
from jax.experimental import pallas as pl
from jax.experimental.pallas import tpu as pltpu
from jax.sharding import PartitionSpec as P

TSHIFT = 2048
TIME_STEP = 0.125
LOG2 = math.log(2.0)
WIDE = 256
CHUNK = 128
TAIL = 16
STRIP = 128
LANES = 128
DET = 3
CHANNELS = 6
SPAN = 68
TERMS = 16
PAYLOAD = CHANNELS * SPAN + DET * TERMS
MEET = 0.75
VMEM = pl.BlockSpec(memory_space=pltpu.VMEM)
F32, BF16 = jnp.float32, jnp.bfloat16


def fit(function, terms):
    nodes = 0.125 * (1.0 + np.cos((np.arange(64) + 0.5) * np.pi / 64))
    basis = np.vander(nodes / 0.25, terms, increasing=True)
    found = np.linalg.lstsq(basis, function(np.sqrt(nodes)), rcond=None)[0]
    return [float(c) for c in found / 0.25 ** np.arange(terms)]


COS = fit(lambda r: np.cos(np.pi * r), 7)
SIN = fit(lambda r: np.sin(np.pi * r) / r, 6)


def horner(coefficients, x):
    total = jnp.full_like(x, coefficients[-1])
    for c in coefficients[-2::-1]:
        total = total * x + c
    return total


def turn(u):
    r = u - jnp.round(u)
    square = r * r
    cosine, sine = horner(COS, square), horner(SIN, square) * r
    twice = sine + sine
    return 1.0 - twice * sine, twice * cosine


def call(kernel, outs, *args, scratch=(), pinned=False, limit=24 << 20, flops=1 << 20, name=None):
    where = VMEM
    if pinned:
        where = pl.BlockSpec(memory_space=pltpu.HBM)
        args = [pltpu.with_memory_space_constraint(a, pltpu.HBM) for a in args]
    return pl.pallas_call(
        kernel,
        out_shape=outs,
        in_specs=[where] * len(args),
        out_specs=jax.tree.map(lambda _: VMEM, outs),
        scratch_shapes=scratch,
        compiler_params=pltpu.CompilerParams(vmem_limit_bytes=limit),
        cost_estimate=pl.CostEstimate(flops=flops, bytes_accessed=1 << 20, transcendentals=0),
        name=name,
    )(*args)


def landing(args):
    return [pltpu.VMEM(a.shape, a.dtype) for a in args] + [pltpu.SemaphoreType.DMA((len(args),))]


def fetch(sources, targets, semaphores):
    copies = [
        pltpu.make_async_copy(source, target, semaphores.at[i])
        for i, (source, target) in enumerate(zip(sources, targets))
    ]
    for copy in copies:
        copy.start()
    return copies


def shifted(x, amount):
    for bit in range(LANES.bit_length() - 1):
        x = jnp.where((amount >> bit) & 1 == 1, pltpu.roll(x, 1 << bit, 1), x)
    return x


def series():
    return [
        (-4.0 * c * math.comb(n, j), n - j, j)
        for n, c in ((2, 1.0), (4, -1.0 / 3), (6, 2.0 / 45))
        for j in range(n + 1)
    ]


def powers(x, count):
    found = [None, x]
    while len(found) <= count:
        found.append(found[-1] * x)
    return found


def monomial(left, right, i, j):
    if i and j:
        return left[i] * right[j]
    return left[i] if i else right[j]


def edges(widths):
    wide = widths.astype(F32)
    bins = wide.shape[1]
    before = lax.broadcasted_iota(jnp.int32, (bins, bins), 0)
    mine = lax.broadcasted_iota(jnp.int32, (bins, bins), 1)
    ones = jnp.where(before <= mine, 1.0, 0.0).astype(BF16)
    rows = jnp.broadcast_to(wide, (16, bins)).astype(BF16)
    upper = jnp.dot(rows, ones, preferred_element_type=F32)[:1]
    return wide, upper


def split(x):
    high = x.astype(BF16)
    return high, (x - high.astype(F32)).astype(BF16)


def summary_kernel(
    cross_in, power_in, widths_in, out_ref, cross_ref, power_ref, widths_ref, sems, grid=0.0
):
    for copy in fetch(
        (widths_in, cross_in, power_in), (widths_ref, cross_ref, power_ref), sems
    ):
        copy.wait()
    fine, bins = power_ref.shape[1], widths_ref.shape[1]
    wide, upper = edges(widths_ref[...])
    lower = upper - wide
    first = (lax.axis_index("draw") * fine).astype(F32)
    at = lax.broadcasted_iota(jnp.int32, (fine, bins), 0).astype(F32) + first
    inside = (at >= lower) & (at < upper)
    up = jnp.where(inside, 2.0 * (at - lower) + 1.0, 0.0)
    down = jnp.where(inside, 2.0 * wide - up, 0.0)
    both_high, both_low = split(up * down)
    weights = jnp.concatenate([up.astype(BF16), down.astype(BF16), both_high, both_low], axis=1)
    data = jnp.concatenate(
        [cross_ref[d] for d in range(DET)] + [power_ref[...], jnp.zeros((7, fine), F32)], axis=0
    )
    high = data.astype(BF16)
    rest = data - high.astype(F32)
    middle, low = split(rest)
    got = jnp.dot(
        jnp.concatenate([high, middle, low], axis=0), weights, preferred_element_type=F32
    )
    got = got[:16] + got[16:32] + got[32:]
    scale = 0.5 / wide
    end = got[:, :bins] * scale
    start = got[:, bins : 2 * bins] * scale
    mixed = (got[:, 2 * bins : 3 * bins] + got[:, 3 * bins :]) * (scale * scale)
    row = lax.broadcasted_iota(jnp.int32, (16, bins), 0)
    lane = lax.broadcasted_iota(jnp.int32, (16, bins), 1)
    merged = end + pltpu.roll(start, bins - 1, 1)
    passed = jnp.sum(jnp.where(upper <= first, 1, 0), axis=1, keepdims=True)
    table = shifted(merged, (bins + 1 - passed) % bins)
    width, x = wide * (1.0 / grid), upper * (1.0 / grid)
    slope = powers(math.pi * width, 6)
    bend = powers(0.5 * width * (x + (x - width)), 6)
    factors = [c * monomial(slope, bend, i, j) for c, i, j in series()]
    factors = jnp.concatenate(factors + [jnp.zeros((1, bins), F32)], axis=0)
    extra = jnp.zeros((TERMS, bins), F32)
    total = jnp.sum(data, axis=1, keepdims=True)
    for d in range(DET):
        each = jnp.sum(factors * mixed[6 + d : 7 + d], axis=1, keepdims=True)
        each = jnp.where(row[:, :1] == TERMS - 1, total[6 + d : 7 + d], each)
        extra = jnp.where(lane == row + (CHANNELS * SPAN % bins + d * TERMS), each, extra)
    tiles = [jnp.zeros((1, bins), F32)] * 4
    tiles[3] = jnp.sum(extra, axis=0, keepdims=True)
    lane = lane[:1]
    for c in range(CHANNELS):
        tile, off = divmod(c * SPAN, bins)
        line = pltpu.roll(table[c : c + 1], off, 1) if off else table[c : c + 1]
        tiles[tile] = tiles[tile] + jnp.where(lane >= off, line, 0.0)
        if off + SPAN > bins:
            tiles[tile + 1] = tiles[tile + 1] + jnp.where(lane < off, line, 0.0)
    for r, tile in enumerate(tiles):
        end = min((r + 1) * bins, PAYLOAD)
        out_ref[:, :, r * bins : end] = jnp.broadcast_to(
            tile[None, :, : end - r * bins], (out_ref.shape[0], 1, end - r * bins)
        )


def terms_kernel(
    widths_in, amps_in, delays_in, phases_in, chirps_in, prior_in,
    cos_ref, sin_ref, features_ref, flat_ref, place_ref,
    widths_ref, amps_ref, delays_ref, phases_ref, chirps_ref, prior_ref, sems,
    grid=0.0, fine=0, start=0,
):
    copies = fetch(
        (widths_in, amps_in, delays_in, phases_in, chirps_in, prior_in),
        (widths_ref, amps_ref, delays_ref, phases_ref, chirps_ref, prior_ref),
        sems,
    )
    copies[0].wait()
    wide, upper = edges(widths_ref[...])
    bins = wide.shape[1]
    draws = features_ref.shape[2]
    mine = pl.ds(pl.multiple_of(lax.axis_index("bin") * draws, draws), draws)
    member = lax.broadcasted_iota(jnp.int32, place_ref.shape, 0)
    source = (member + start) % place_ref.shape[0] * fine
    passed = jnp.sum(jnp.where(upper <= source.astype(F32), 1, 0), axis=1, keepdims=True)
    place_ref[...] = jnp.broadcast_to((passed + (bins - 1)) % bins, place_ref.shape)
    step = upper * (TIME_STEP / grid)
    near = lax.broadcasted_iota(jnp.int32, (CHUNK, bins), 0).astype(F32)
    near_cos, near_sin = turn(near * step)
    for first in range(0, TSHIFT // 2 + TAIL, CHUNK):
        size = min(CHUNK, TSHIFT // 2 + TAIL - first)
        rows = slice(first, first + size)
        far_cos, far_sin = turn(float(first) * step)
        here_cos, here_sin = near_cos[:size], near_sin[:size]
        cosine = here_cos * far_cos - here_sin * far_sin
        sine = here_sin * far_cos + here_cos * far_sin
        cos_ref[rows, :bins], cos_ref[rows, bins:] = split(cosine)
        sin_ref[rows, :bins], sin_ref[rows, bins:] = split(sine)
    tall = jnp.concatenate([upper, jnp.zeros((bins - 1, bins), F32)], axis=0).T
    x = tall[:, :1] * (1.0 / grid)
    for copy in copies[1:]:
        copy.wait()
    chirps = chirps_ref[:, mine]
    base = phases_ref[:, mine] * (0.5 / math.pi)
    common = base + (chirps * (0.5 / math.pi)) * (x * x)
    cos0, sin0 = turn(base)
    for d in range(DET):
        amp = jnp.exp(amps_ref[d : d + 1, mine])
        delay = delays_ref[d : d + 1, mine]
        cosine, sine = turn(x * delay + common)
        features_ref[2 * d] = amp * cosine
        features_ref[2 * d + 1] = amp * sine
        flat_ref[2 * d : 2 * d + 1] = amp * cos0
        flat_ref[2 * d + 1 : 2 * d + 2] = amp * sin0
    flat_ref[6:7] = prior_ref[:, mine]
    flat_ref[7:8] = chirps
    flat_ref[8 : 8 + DET] = delays_ref[:, mine]
    flat_ref[8 + DET :] = jnp.zeros((8 - DET, draws), F32)


def score_kernel(
    sums_ref, cos_ref, sin_ref, features_ref, flat_ref, place_ref, out_ref, stat_ref,
    zero=0,
):
    bins = features_ref.shape[1]
    draws = features_ref.shape[2]
    half = TSHIFT // 2
    place = place_ref[...]
    row = lax.broadcasted_iota(jnp.int32, place.shape, 0)
    lane = lax.broadcasted_iota(jnp.int32, place.shape, 1)
    tiles = [sums_ref[:, 0, r * bins : (r + 1) * bins] for r in range(3)]
    last = sums_ref[:, 0, 3 * bins : PAYLOAD]
    rest = jnp.zeros((last.shape[0], 4 * bins - PAYLOAD), F32)
    tiles.append(jnp.concatenate([last, rest], axis=1))
    lines, single = [], []
    for c in range(CHANNELS):
        tile, off = divmod(c * SPAN, bins)
        line = pltpu.roll(tiles[tile], bins - off, 1) if off else tiles[tile]
        if off + SPAN > bins:
            line = jnp.where(lane < bins - off, line, pltpu.roll(tiles[tile + 1], bins - off, 1))
        line = shifted(jnp.where(lane < SPAN, line, 0.0), place)
        single.append(line[zero : zero + 1, bins - 1 :])
        line = jnp.where((row == zero) & (lane == bins - 1), 0.0, line)
        lines.append(jnp.sum(line, axis=0, keepdims=True))
    tall = jnp.concatenate(lines + [jnp.zeros((bins - CHANNELS, bins), F32)], axis=0).T
    extra = jnp.sum(tiles[3], axis=0, keepdims=True)
    extra = [
        pltpu.roll(extra, bins - CHANNELS * SPAN % bins - d * TERMS, 1) for d in range(DET)
    ]
    extra = jnp.concatenate(extra + [jnp.zeros((8 - DET, bins), F32)], axis=0)
    chirp = powers(jnp.broadcast_to(flat_ref[7:8], (8, draws)), 6)
    delay = powers(flat_ref[8:], 6)
    power = jnp.broadcast_to(extra[:, TERMS - 1 : TERMS], (8, draws))
    for k, (_, i, j) in enumerate(series()):
        power = power + extra[:, k : k + 1] * monomial(delay, chirp, i, j)
    real = imag = None
    offset = flat_ref[6:7]
    for d in range(DET):
        a, b = tall[:, 2 * d : 2 * d + 1], tall[:, 2 * d + 1 : 2 * d + 2]
        cosine, sine = features_ref[2 * d], features_ref[2 * d + 1]
        re, im = a * cosine + b * sine, b * cosine - a * sine
        real = re if real is None else real + re
        imag = im if imag is None else imag + im
        cos0, sin0 = flat_ref[2 * d : 2 * d + 1], flat_ref[2 * d + 1 : 2 * d + 2]
        offset = offset + single[2 * d] * cos0 + single[2 * d + 1] * sin0
        offset = offset - (0.5 * power[d : d + 1]) * (cos0 * cos0 + sin0 * sin0)
    real, imag = (
        [jnp.concatenate([piece, piece], axis=0) for piece in split(part * (1.0 / LOG2))]
        for part in (real, imag)
    )

    def rotated(rows, columns):
        return (
            jnp.dot(ref[rows, :], part[0][:, columns], preferred_element_type=F32)
            + jnp.dot(ref[rows, :], part[1][:, columns], preferred_element_type=F32)
            for ref, part in ((cos_ref, real), (sin_ref, imag))
        )

    marginal = []
    for start in range(0, draws, WIDE):
        columns = slice(start, start + WIDE)
        even, odd = rotated(slice(half, half + TAIL), columns)
        earliest = (even - odd)[:1]
        top = total = None
        for first in range(0, half, STRIP):
            even, odd = rotated(slice(first, first + STRIP), columns)
            after, before = even + odd, even - odd
            if first == 0:
                at = lax.broadcasted_iota(jnp.int32, before.shape, 0)
                before = jnp.where(at == 0, earliest, before)
            after = after.reshape(STRIP // 8, 8, WIDE)
            before = before.reshape(STRIP // 8, 8, WIDE)
            peak = jnp.max(jnp.maximum(after, before), axis=0)
            if top is not None:
                peak = jnp.maximum(peak, top)
                total = total * jnp.exp2(top - peak)
            add = jnp.sum(jnp.exp2(after - peak[None]) + jnp.exp2(before - peak[None]), axis=0)
            total = add if total is None else total + add
            top = peak
        peak = jnp.max(top, axis=0, keepdims=True)
        total = jnp.sum(total * jnp.exp2(top - peak), axis=0, keepdims=True)
        marginal.append(peak * LOG2 + (jnp.log(total) - math.log(TSHIFT)))
    marginal = jnp.concatenate(marginal, axis=1) + offset
    out_ref[...] = marginal
    best = jnp.max(marginal, axis=1, keepdims=True)
    mass = jnp.sum(jnp.exp(marginal - best), axis=1, keepdims=True)
    lane = lax.broadcasted_iota(jnp.int32, (1, LANES), 1)
    stat = jnp.where(lane == 0, best, mass)
    stat_ref[...] = jnp.broadcast_to(stat[None], stat_ref.shape)


def final_kernel(stats_ref, marginal_ref, out_ref, evidence_ref, draws=0):
    stats = stats_ref[...]
    best, mass = stats[:, :, :1], stats[:, :, 1:2]
    top = jnp.max(best, axis=0, keepdims=True)
    total = top + jnp.log(jnp.sum(mass * jnp.exp(best - top), axis=0, keepdims=True))
    out_ref[...] = marginal_ref[...] - total
    evidence_ref[...] = total[0] - math.log(draws)


def body(fine_cross, fine_power, bin_widths, log_amps, delays, phases, chirps, proposal_log):
    shards, cores = lax.axis_size("draw"), lax.axis_size("bin")
    detectors, fine = fine_power.shape
    bins = bin_widths.shape[0]
    whole = log_amps.shape[1]
    draws = whole // cores
    widths = bin_widths.reshape(1, bins)
    turned = [(i + int(shards * MEET)) % shards for i in range(shards)]
    args = (fine_cross, fine_power, widths)
    sums = call(
        functools.partial(summary_kernel, grid=float(fine * shards)),
        jax.ShapeDtypeStruct((shards, 1, PAYLOAD), F32),
        *args, scratch=landing(args), pinned=True, flops=1 << 24, name="summary",
    )
    everyone = lax.all_to_all(sums, "draw", 0, 0, axis_index_groups=[turned], tiled=True)
    args = (
        widths, log_amps, delays, phases.reshape(1, whole), chirps.reshape(1, whole),
        proposal_log.reshape(1, whole),
    )
    terms = call(
        functools.partial(terms_kernel, grid=float(fine * shards), fine=fine, start=turned[0]),
        (
            jax.ShapeDtypeStruct((TSHIFT // 2 + TAIL, 2 * bins), BF16),
            jax.ShapeDtypeStruct((TSHIFT // 2 + TAIL, 2 * bins), BF16),
            jax.ShapeDtypeStruct((2 * detectors, bins, draws), F32),
            jax.ShapeDtypeStruct((16, draws), F32),
            jax.ShapeDtypeStruct((shards, bins), jnp.int32),
        ),
        *args, scratch=landing(args), pinned=True, flops=1 << 28, name="terms",
    )
    marginal, stat = call(
        functools.partial(score_kernel, zero=turned.index(0)),
        (
            jax.ShapeDtypeStruct((1, draws), F32),
            jax.ShapeDtypeStruct((shards * cores, 1, LANES), F32),
        ),
        everyone, *terms, flops=1 << 30, name="score",
    )
    both = [i * cores + c for i in turned for c in range(cores)]
    stats = lax.all_to_all(
        stat, ("draw", "bin"), 0, 0, axis_index_groups=[both], tiled=True
    )
    marginals = lax.all_gather(marginal.reshape(1, 1, draws), "bin", axis=0, tiled=True)
    weights, evidence = call(
        lambda *refs: final_kernel(*refs, draws=whole * shards),
        (
            jax.ShapeDtypeStruct((cores, 1, draws), F32),
            jax.ShapeDtypeStruct((1, 1), F32),
        ),
        stats, marginals, name="final",
    )
    return weights.reshape(whole), evidence.reshape(1)


def solution(mesh):
    placed = (
        P("event", None, "draw"),
        P("event", "draw"),
        P("event"),
        P("event", "draw"),
        P("event", "draw"),
        P(("event", "draw")),
        P(("event", "draw")),
        P(("event", "draw")),
    )
    return jax.shard_map(
        body,
        mesh=mesh,
        in_specs=placed,
        out_specs=(P(("event", "draw")), P("event")),
        check_vma=False,
    )
```

```python
import functools
import math

import jax
import jax.numpy as jnp
import numpy as np
from jax import lax
from jax.experimental import pallas as pl
from jax.experimental.pallas import tpu as pltpu
from jax.sharding import PartitionSpec as P

TSHIFT = 2048
TIME_STEP = 0.125
LOG2 = math.log(2.0)
WIDE = 256
CHUNK = 128
TAIL = 16
STRIP = 128
LANES = 128
DET = 3
CHANNELS = 6
SPAN = 68
TERMS = 16
PAYLOAD = CHANNELS * SPAN + DET * TERMS
MEET = 0.75
VMEM = pl.BlockSpec(memory_space=pltpu.VMEM)
F32, BF16 = jnp.float32, jnp.bfloat16


def fit(function, terms):
    nodes = 0.125 * (1.0 + np.cos((np.arange(64) + 0.5) * np.pi / 64))
    basis = np.vander(nodes / 0.25, terms, increasing=True)
    found = np.linalg.lstsq(basis, function(np.sqrt(nodes)), rcond=None)[0]
    return [float(c) for c in found / 0.25 ** np.arange(terms)]


COS = fit(lambda r: np.cos(np.pi * r), 7)
SIN = fit(lambda r: np.sin(np.pi * r) / r, 6)


def horner(coefficients, x):
    total = jnp.full_like(x, coefficients[-1])
    for c in coefficients[-2::-1]:
        total = total * x + c
    return total


def turn(u):
    r = u - jnp.round(u)
    square = r * r
    cosine, sine = horner(COS, square), horner(SIN, square) * r
    twice = sine + sine
    return 1.0 - twice * sine, twice * cosine


def call(kernel, outs, *args, scratch=(), pinned=False, limit=24 << 20, flops=1 << 20, name=None):
    where = VMEM
    if pinned:
        where = pl.BlockSpec(memory_space=pltpu.HBM)
        args = [pltpu.with_memory_space_constraint(a, pltpu.HBM) for a in args]
    return pl.pallas_call(
        kernel,
        out_shape=outs,
        in_specs=[where] * len(args),
        out_specs=jax.tree.map(lambda _: VMEM, outs),
        scratch_shapes=scratch,
        compiler_params=pltpu.CompilerParams(vmem_limit_bytes=limit),
        cost_estimate=pl.CostEstimate(flops=flops, bytes_accessed=1 << 20, transcendentals=0),
        name=name,
    )(*args)


def landing(args):
    return [pltpu.VMEM(a.shape, a.dtype) for a in args] + [pltpu.SemaphoreType.DMA((len(args),))]


def fetch(sources, targets, semaphores):
    copies = [
        pltpu.make_async_copy(source, target, semaphores.at[i])
        for i, (source, target) in enumerate(zip(sources, targets))
    ]
    for copy in copies:
        copy.start()
    return copies


def shifted(x, amount):
    for bit in range(LANES.bit_length() - 1):
        x = jnp.where((amount >> bit) & 1 == 1, pltpu.roll(x, 1 << bit, 1), x)
    return x


def series():
    return [
        (-4.0 * c * math.comb(n, j), n - j, j)
        for n, c in ((2, 1.0), (4, -1.0 / 3), (6, 2.0 / 45))
        for j in range(n + 1)
    ]


def powers(x, count):
    found = [None, x]
    while len(found) <= count:
        found.append(found[-1] * x)
    return found


def monomial(left, right, i, j):
    if i and j:
        return left[i] * right[j]
    return left[i] if i else right[j]


def edges(widths):
    wide = widths.astype(F32)
    bins = wide.shape[1]
    before = lax.broadcasted_iota(jnp.int32, (bins, bins), 0)
    mine = lax.broadcasted_iota(jnp.int32, (bins, bins), 1)
    ones = jnp.where(before <= mine, 1.0, 0.0).astype(BF16)
    rows = jnp.broadcast_to(wide, (16, bins)).astype(BF16)
    upper = jnp.dot(rows, ones, preferred_element_type=F32)[:1]
    return wide, upper


def split(x):
    high = x.astype(BF16)
    return high, (x - high.astype(F32)).astype(BF16)


def summary_kernel(
    cross_in, power_in, widths_in, out_ref, cross_ref, power_ref, widths_ref, sems, grid=0.0
):
    for copy in fetch(
        (widths_in, cross_in, power_in), (widths_ref, cross_ref, power_ref), sems
    ):
        copy.wait()
    fine, bins = power_ref.shape[1], widths_ref.shape[1]
    wide, upper = edges(widths_ref[...])
    lower = upper - wide
    first = (lax.axis_index("draw") * fine).astype(F32)
    at = lax.broadcasted_iota(jnp.int32, (fine, bins), 0).astype(F32) + first
    inside = (at >= lower) & (at < upper)
    up = jnp.where(inside, 2.0 * (at - lower) + 1.0, 0.0)
    down = jnp.where(inside, 2.0 * wide - up, 0.0)
    both_high, both_low = split(up * down)
    weights = jnp.concatenate([up.astype(BF16), down.astype(BF16), both_high, both_low], axis=1)
    data = jnp.concatenate(
        [cross_ref[d] for d in range(DET)] + [power_ref[...], jnp.zeros((7, fine), F32)], axis=0
    )
    high = data.astype(BF16)
    rest = data - high.astype(F32)
    middle, low = split(rest)
    got = jnp.dot(
        jnp.concatenate([high, middle, low], axis=0), weights, preferred_element_type=F32
    )
    got = got[:16] + got[16:32] + got[32:]
    scale = 0.5 / wide
    end = got[:, :bins] * scale
    start = got[:, bins : 2 * bins] * scale
    mixed = (got[:, 2 * bins : 3 * bins] + got[:, 3 * bins :]) * (scale * scale)
    row = lax.broadcasted_iota(jnp.int32, (16, bins), 0)
    lane = lax.broadcasted_iota(jnp.int32, (16, bins), 1)
    merged = end + pltpu.roll(start, bins - 1, 1)
    passed = jnp.sum(jnp.where(upper <= first, 1, 0), axis=1, keepdims=True)
    table = shifted(merged, (bins + 1 - passed) % bins)
    width, x = wide * (1.0 / grid), upper * (1.0 / grid)
    slope = powers(math.pi * width, 6)
    bend = powers(0.5 * width * (x + (x - width)), 6)
    factors = [c * monomial(slope, bend, i, j) for c, i, j in series()]
    factors = jnp.concatenate(factors + [jnp.zeros((1, bins), F32)], axis=0)
    extra = jnp.zeros((TERMS, bins), F32)
    total = jnp.sum(data, axis=1, keepdims=True)
    for d in range(DET):
        each = jnp.sum(factors * mixed[6 + d : 7 + d], axis=1, keepdims=True)
        each = jnp.where(row[:, :1] == TERMS - 1, total[6 + d : 7 + d], each)
        extra = jnp.where(lane == row + (CHANNELS * SPAN % bins + d * TERMS), each, extra)
    tiles = [jnp.zeros((1, bins), F32)] * 4
    tiles[3] = jnp.sum(extra, axis=0, keepdims=True)
    lane = lane[:1]
    for c in range(CHANNELS):
        tile, off = divmod(c * SPAN, bins)
        line = pltpu.roll(table[c : c + 1], off, 1) if off else table[c : c + 1]
        tiles[tile] = tiles[tile] + jnp.where(lane >= off, line, 0.0)
        if off + SPAN > bins:
            tiles[tile + 1] = tiles[tile + 1] + jnp.where(lane < off, line, 0.0)
    for r, tile in enumerate(tiles):
        end = min((r + 1) * bins, PAYLOAD)
        out_ref[:, :, r * bins : end] = jnp.broadcast_to(
            tile[None, :, : end - r * bins], (out_ref.shape[0], 1, end - r * bins)
        )


def terms_kernel(
    widths_in, amps_in, delays_in, phases_in, chirps_in, prior_in,
    cos_ref, sin_ref, features_ref, flat_ref, place_ref,
    widths_ref, amps_ref, delays_ref, phases_ref, chirps_ref, prior_ref, sems,
    grid=0.0, fine=0, start=0,
):
    copies = fetch(
        (widths_in, amps_in, delays_in, phases_in, chirps_in, prior_in),
        (widths_ref, amps_ref, delays_ref, phases_ref, chirps_ref, prior_ref),
        sems,
    )
    copies[0].wait()
    wide, upper = edges(widths_ref[...])
    bins = wide.shape[1]
    draws = features_ref.shape[2]
    mine = pl.ds(pl.multiple_of(lax.axis_index("bin") * draws, draws), draws)
    member = lax.broadcasted_iota(jnp.int32, place_ref.shape, 0)
    source = (member + start) % place_ref.shape[0] * fine
    passed = jnp.sum(jnp.where(upper <= source.astype(F32), 1, 0), axis=1, keepdims=True)
    place_ref[...] = jnp.broadcast_to((passed + (bins - 1)) % bins, place_ref.shape)
    step = upper * (TIME_STEP / grid)
    near = lax.broadcasted_iota(jnp.int32, (CHUNK, bins), 0).astype(F32)
    near_cos, near_sin = turn(near * step)
    for first in range(0, TSHIFT // 2 + TAIL, CHUNK):
        size = min(CHUNK, TSHIFT // 2 + TAIL - first)
        rows = slice(first, first + size)
        far_cos, far_sin = turn(float(first) * step)
        here_cos, here_sin = near_cos[:size], near_sin[:size]
        cosine = here_cos * far_cos - here_sin * far_sin
        sine = here_sin * far_cos + here_cos * far_sin
        cos_ref[rows, :bins], cos_ref[rows, bins:] = split(cosine)
        sin_ref[rows, :bins], sin_ref[rows, bins:] = split(sine)
    tall = jnp.concatenate([upper, jnp.zeros((bins - 1, bins), F32)], axis=0).T
    x = tall[:, :1] * (1.0 / grid)
    for copy in copies[1:]:
        copy.wait()
    chirps = chirps_ref[:, mine]
    base = phases_ref[:, mine] * (0.5 / math.pi)
    common = base + (chirps * (0.5 / math.pi)) * (x * x)
    cos0, sin0 = turn(base)
    for d in range(DET):
        amp = jnp.exp(amps_ref[d : d + 1, mine])
        delay = delays_ref[d : d + 1, mine]
        cosine, sine = turn(x * delay + common)
        features_ref[2 * d] = amp * cosine
        features_ref[2 * d + 1] = amp * sine
        flat_ref[2 * d : 2 * d + 1] = amp * cos0
        flat_ref[2 * d + 1 : 2 * d + 2] = amp * sin0
    flat_ref[6:7] = prior_ref[:, mine]
    flat_ref[7:8] = chirps
    flat_ref[8 : 8 + DET] = delays_ref[:, mine]
    flat_ref[8 + DET :] = jnp.zeros((8 - DET, draws), F32)


def score_kernel(
    sums_ref, cos_ref, sin_ref, features_ref, flat_ref, place_ref, out_ref, stat_ref,
    zero=0,
):
    bins = features_ref.shape[1]
    draws = features_ref.shape[2]
    half = TSHIFT // 2
    place = place_ref[...]
    row = lax.broadcasted_iota(jnp.int32, place.shape, 0)
    lane = lax.broadcasted_iota(jnp.int32, place.shape, 1)
    tiles = [sums_ref[:, 0, r * bins : (r + 1) * bins] for r in range(3)]
    last = sums_ref[:, 0, 3 * bins : PAYLOAD]
    rest = jnp.zeros((last.shape[0], 4 * bins - PAYLOAD), F32)
    tiles.append(jnp.concatenate([last, rest], axis=1))
    lines, single = [], []
    for c in range(CHANNELS):
        tile, off = divmod(c * SPAN, bins)
        line = pltpu.roll(tiles[tile], bins - off, 1) if off else tiles[tile]
        if off + SPAN > bins:
            line = jnp.where(lane < bins - off, line, pltpu.roll(tiles[tile + 1], bins - off, 1))
        line = shifted(jnp.where(lane < SPAN, line, 0.0), place)
        single.append(line[zero : zero + 1, bins - 1 :])
        line = jnp.where((row == zero) & (lane == bins - 1), 0.0, line)
        lines.append(jnp.sum(line, axis=0, keepdims=True))
    tall = jnp.concatenate(lines + [jnp.zeros((bins - CHANNELS, bins), F32)], axis=0).T
    extra = jnp.sum(tiles[3], axis=0, keepdims=True)
    extra = [
        pltpu.roll(extra, bins - CHANNELS * SPAN % bins - d * TERMS, 1) for d in range(DET)
    ]
    extra = jnp.concatenate(extra + [jnp.zeros((8 - DET, bins), F32)], axis=0)
    chirp = powers(jnp.broadcast_to(flat_ref[7:8], (8, draws)), 6)
    delay = powers(flat_ref[8:], 6)
    power = jnp.broadcast_to(extra[:, TERMS - 1 : TERMS], (8, draws))
    for k, (_, i, j) in enumerate(series()):
        power = power + extra[:, k : k + 1] * monomial(delay, chirp, i, j)
    real = imag = None
    offset = flat_ref[6:7]
    for d in range(DET):
        a, b = tall[:, 2 * d : 2 * d + 1], tall[:, 2 * d + 1 : 2 * d + 2]
        cosine, sine = features_ref[2 * d], features_ref[2 * d + 1]
        re, im = a * cosine + b * sine, b * cosine - a * sine
        real = re if real is None else real + re
        imag = im if imag is None else imag + im
        cos0, sin0 = flat_ref[2 * d : 2 * d + 1], flat_ref[2 * d + 1 : 2 * d + 2]
        offset = offset + single[2 * d] * cos0 + single[2 * d + 1] * sin0
        offset = offset - (0.5 * power[d : d + 1]) * (cos0 * cos0 + sin0 * sin0)
    real, imag = (
        [jnp.concatenate([piece, piece], axis=0) for piece in split(part * (1.0 / LOG2))]
        for part in (real, imag)
    )

    def rotated(rows, columns):
        return (
            jnp.dot(ref[rows, :], part[0][:, columns], preferred_element_type=F32)
            + jnp.dot(ref[rows, :], part[1][:, columns], preferred_element_type=F32)
            for ref, part in ((cos_ref, real), (sin_ref, imag))
        )

    marginal = []
    for start in range(0, draws, WIDE):
        columns = slice(start, start + WIDE)
        even, odd = rotated(slice(half, half + TAIL), columns)
        earliest = (even - odd)[:1]
        top = total = None
        for first in range(0, half, STRIP):
            even, odd = rotated(slice(first, first + STRIP), columns)
            after, before = even + odd, even - odd
            if first == 0:
                at = lax.broadcasted_iota(jnp.int32, before.shape, 0)
                before = jnp.where(at == 0, earliest, before)
            after = after.reshape(STRIP // 8, 8, WIDE)
            before = before.reshape(STRIP // 8, 8, WIDE)
            peak = jnp.max(jnp.maximum(after, before), axis=0)
            if top is not None:
                peak = jnp.maximum(peak, top)
                total = total * jnp.exp2(top - peak)
            add = jnp.sum(jnp.exp2(after - peak[None]) + jnp.exp2(before - peak[None]), axis=0)
            total = add if total is None else total + add
            top = peak
        peak = jnp.max(top, axis=0, keepdims=True)
        total = jnp.sum(total * jnp.exp2(top - peak), axis=0, keepdims=True)
        marginal.append(peak * LOG2 + (jnp.log(total) - math.log(TSHIFT)))
    marginal = jnp.concatenate(marginal, axis=1) + offset
    out_ref[...] = marginal
    best = jnp.max(marginal, axis=1, keepdims=True)
    mass = jnp.sum(jnp.exp(marginal - best), axis=1, keepdims=True)
    lane = lax.broadcasted_iota(jnp.int32, (1, LANES), 1)
    stat = jnp.where(lane == 0, best, mass)
    stat_ref[...] = jnp.broadcast_to(stat[None], stat_ref.shape)


def merged(stats):
    best, mass = stats[:, :, :1], stats[:, :, 1:2]
    top = jnp.max(best, axis=0, keepdims=True)
    return top, jnp.sum(mass * jnp.exp(best - top), axis=0, keepdims=True)


def half_kernel(stats_ref, out_ref):
    top, mass = merged(stats_ref[...])
    lane = lax.broadcasted_iota(jnp.int32, out_ref.shape, 2)
    out_ref[...] = jnp.where(lane == 0, top, mass)


def final_kernel(stats_ref, marginal_ref, out_ref, evidence_ref, draws=0):
    top, mass = merged(stats_ref[...])
    total = top + jnp.log(mass)
    out_ref[...] = marginal_ref[...] - total
    evidence_ref[...] = total[0] - math.log(draws)


def body(fine_cross, fine_power, bin_widths, log_amps, delays, phases, chirps, proposal_log):
    shards, cores = lax.axis_size("draw"), lax.axis_size("bin")
    detectors, fine = fine_power.shape
    bins = bin_widths.shape[0]
    whole = log_amps.shape[1]
    draws = whole // cores
    widths = bin_widths.reshape(1, bins)
    turned = [(i + int(shards * MEET)) % shards for i in range(shards)]
    args = (fine_cross, fine_power, widths)
    sums = call(
        functools.partial(summary_kernel, grid=float(fine * shards)),
        jax.ShapeDtypeStruct((shards, 1, PAYLOAD), F32),
        *args, scratch=landing(args), pinned=True, flops=1 << 24, name="summary",
    )
    everyone = lax.all_to_all(sums, "draw", 0, 0, axis_index_groups=[turned], tiled=True)
    args = (
        widths, log_amps, delays, phases.reshape(1, whole), chirps.reshape(1, whole),
        proposal_log.reshape(1, whole),
    )
    terms = call(
        functools.partial(terms_kernel, grid=float(fine * shards), fine=fine, start=turned[0]),
        (
            jax.ShapeDtypeStruct((TSHIFT // 2 + TAIL, 2 * bins), BF16),
            jax.ShapeDtypeStruct((TSHIFT // 2 + TAIL, 2 * bins), BF16),
            jax.ShapeDtypeStruct((2 * detectors, bins, draws), F32),
            jax.ShapeDtypeStruct((16, draws), F32),
            jax.ShapeDtypeStruct((shards, bins), jnp.int32),
        ),
        *args, scratch=landing(args), pinned=True, flops=1 << 28, name="terms",
    )
    marginal, stat = call(
        functools.partial(score_kernel, zero=turned.index(0)),
        (
            jax.ShapeDtypeStruct((1, draws), F32),
            jax.ShapeDtypeStruct((shards, 1, LANES), F32),
        ),
        everyone, *terms, flops=1 << 30, name="score",
    )
    stats = lax.all_to_all(stat, "draw", 0, 0, axis_index_groups=[turned], tiled=True)
    marginals = lax.all_gather(marginal.reshape(1, 1, draws), "bin", axis=0, tiled=True)
    half = call(half_kernel, jax.ShapeDtypeStruct((1, 1, LANES), F32), stats, name="half")
    halves = lax.all_gather(half, "bin", axis=0, tiled=True)
    weights, evidence = call(
        lambda *refs: final_kernel(*refs, draws=whole * shards),
        (
            jax.ShapeDtypeStruct((cores, 1, draws), F32),
            jax.ShapeDtypeStruct((1, 1), F32),
        ),
        halves, marginals, name="final",
    )
    return weights.reshape(whole), evidence.reshape(1)


def solution(mesh):
    placed = (
        P("event", None, "draw"),
        P("event", "draw"),
        P("event"),
        P("event", "draw"),
        P("event", "draw"),
        P(("event", "draw")),
        P(("event", "draw")),
        P(("event", "draw")),
    )
    return jax.shard_map(
        body,
        mesh=mesh,
        in_specs=placed,
        out_specs=(P(("event", "draw")), P("event")),
        check_vma=False,
    )
```

```python
import functools
import math

import jax
import jax.numpy as jnp
import numpy as np
from jax import lax
from jax.experimental import pallas as pl
from jax.experimental.pallas import tpu as pltpu
from jax.sharding import PartitionSpec as P

TSHIFT = 2048
TIME_STEP = 0.125
LOG2 = math.log(2.0)
WIDE = 256
CHUNK = 128
TAIL = 16
STRIP = 128
LANES = 128
DET = 3
CHANNELS = 6
SPAN = 68
TERMS = 16
PAYLOAD = CHANNELS * SPAN + DET * TERMS
MEET = 0.75
VMEM = pl.BlockSpec(memory_space=pltpu.VMEM)
F32, BF16 = jnp.float32, jnp.bfloat16


def fit(function, terms):
    nodes = 0.125 * (1.0 + np.cos((np.arange(64) + 0.5) * np.pi / 64))
    basis = np.vander(nodes / 0.25, terms, increasing=True)
    found = np.linalg.lstsq(basis, function(np.sqrt(nodes)), rcond=None)[0]
    return [float(c) for c in found / 0.25 ** np.arange(terms)]


COS = fit(lambda r: np.cos(np.pi * r), 7)
SIN = fit(lambda r: np.sin(np.pi * r) / r, 6)


def horner(coefficients, x):
    total = jnp.full_like(x, coefficients[-1])
    for c in coefficients[-2::-1]:
        total = total * x + c
    return total


def turn(u):
    r = u - jnp.round(u)
    square = r * r
    cosine, sine = horner(COS, square), horner(SIN, square) * r
    twice = sine + sine
    return 1.0 - twice * sine, twice * cosine


def call(kernel, outs, *args, scratch=(), pinned=False, limit=24 << 20, flops=1 << 20, name=None):
    where = VMEM
    if pinned:
        where = pl.BlockSpec(memory_space=pltpu.HBM)
        args = [pltpu.with_memory_space_constraint(a, pltpu.HBM) for a in args]
    return pl.pallas_call(
        kernel,
        out_shape=outs,
        in_specs=[where] * len(args),
        out_specs=jax.tree.map(lambda _: VMEM, outs),
        scratch_shapes=scratch,
        compiler_params=pltpu.CompilerParams(vmem_limit_bytes=limit),
        cost_estimate=pl.CostEstimate(flops=flops, bytes_accessed=1 << 20, transcendentals=0),
        name=name,
    )(*args)


def landing(args):
    return [pltpu.VMEM(a.shape, a.dtype) for a in args] + [pltpu.SemaphoreType.DMA((len(args),))]


def fetch(sources, targets, semaphores):
    copies = [
        pltpu.make_async_copy(source, target, semaphores.at[i])
        for i, (source, target) in enumerate(zip(sources, targets))
    ]
    for copy in copies:
        copy.start()
    return copies


def shifted(x, amount):
    for bit in range(LANES.bit_length() - 1):
        x = jnp.where((amount >> bit) & 1 == 1, pltpu.roll(x, 1 << bit, 1), x)
    return x


def series():
    return [
        (-4.0 * c * math.comb(n, j), n - j, j)
        for n, c in ((2, 1.0), (4, -1.0 / 3), (6, 2.0 / 45))
        for j in range(n + 1)
    ]


def powers(x, count):
    found = [None, x]
    while len(found) <= count:
        found.append(found[-1] * x)
    return found


def monomial(left, right, i, j):
    if i and j:
        return left[i] * right[j]
    return left[i] if i else right[j]


def edges(widths):
    wide = widths.astype(F32)
    bins = wide.shape[1]
    before = lax.broadcasted_iota(jnp.int32, (bins, bins), 0)
    mine = lax.broadcasted_iota(jnp.int32, (bins, bins), 1)
    ones = jnp.where(before <= mine, 1.0, 0.0).astype(BF16)
    rows = jnp.broadcast_to(wide, (16, bins)).astype(BF16)
    upper = jnp.dot(rows, ones, preferred_element_type=F32)[:1]
    return wide, upper


def split(x):
    high = x.astype(BF16)
    return high, (x - high.astype(F32)).astype(BF16)


def summary_kernel(
    cross_in, power_in, widths_in, out_ref, cross_ref, power_ref, widths_ref, sems, grid=0.0
):
    for copy in fetch(
        (widths_in, cross_in, power_in), (widths_ref, cross_ref, power_ref), sems
    ):
        copy.wait()
    fine, bins = power_ref.shape[1], widths_ref.shape[1]
    wide, upper = edges(widths_ref[...])
    lower = upper - wide
    first = (lax.axis_index("draw") * fine).astype(F32)
    at = lax.broadcasted_iota(jnp.int32, (fine, bins), 0).astype(F32) + first
    inside = (at >= lower) & (at < upper)
    up = jnp.where(inside, 2.0 * (at - lower) + 1.0, 0.0)
    down = jnp.where(inside, 2.0 * wide - up, 0.0)
    both_high, both_low = split(up * down)
    weights = jnp.concatenate([up.astype(BF16), down.astype(BF16), both_high, both_low], axis=1)
    data = jnp.concatenate(
        [cross_ref[d] for d in range(DET)] + [power_ref[...], jnp.zeros((7, fine), F32)], axis=0
    )
    high = data.astype(BF16)
    rest = data - high.astype(F32)
    middle, low = split(rest)
    got = jnp.dot(
        jnp.concatenate([high, middle, low], axis=0), weights, preferred_element_type=F32
    )
    got = got[:16] + got[16:32] + got[32:]
    scale = 0.5 / wide
    end = got[:, :bins] * scale
    start = got[:, bins : 2 * bins] * scale
    mixed = (got[:, 2 * bins : 3 * bins] + got[:, 3 * bins :]) * (scale * scale)
    row = lax.broadcasted_iota(jnp.int32, (16, bins), 0)
    lane = lax.broadcasted_iota(jnp.int32, (16, bins), 1)
    merged = end + pltpu.roll(start, bins - 1, 1)
    passed = jnp.sum(jnp.where(upper <= first, 1, 0), axis=1, keepdims=True)
    table = shifted(merged, (bins + 1 - passed) % bins)
    width, x = wide * (1.0 / grid), upper * (1.0 / grid)
    slope = powers(math.pi * width, 6)
    bend = powers(0.5 * width * (x + (x - width)), 6)
    factors = [c * monomial(slope, bend, i, j) for c, i, j in series()]
    factors = jnp.concatenate(factors + [jnp.zeros((1, bins), F32)], axis=0)
    extra = jnp.zeros((TERMS, bins), F32)
    total = jnp.sum(data, axis=1, keepdims=True)
    for d in range(DET):
        each = jnp.sum(factors * mixed[6 + d : 7 + d], axis=1, keepdims=True)
        each = jnp.where(row[:, :1] == TERMS - 1, total[6 + d : 7 + d], each)
        extra = jnp.where(lane == row + (CHANNELS * SPAN % bins + d * TERMS), each, extra)
    tiles = [jnp.zeros((1, bins), F32)] * 4
    tiles[3] = jnp.sum(extra, axis=0, keepdims=True)
    lane = lane[:1]
    for c in range(CHANNELS):
        tile, off = divmod(c * SPAN, bins)
        line = pltpu.roll(table[c : c + 1], off, 1) if off else table[c : c + 1]
        tiles[tile] = tiles[tile] + jnp.where(lane >= off, line, 0.0)
        if off + SPAN > bins:
            tiles[tile + 1] = tiles[tile + 1] + jnp.where(lane < off, line, 0.0)
    for r, tile in enumerate(tiles):
        end = min((r + 1) * bins, PAYLOAD)
        out_ref[:, :, r * bins : end] = jnp.broadcast_to(
            tile[None, :, : end - r * bins], (out_ref.shape[0], 1, end - r * bins)
        )


def terms_kernel(
    widths_in, amps_in, delays_in, phases_in, chirps_in, prior_in,
    cos_ref, sin_ref, features_ref, flat_ref, place_ref,
    widths_ref, amps_ref, delays_ref, phases_ref, chirps_ref, prior_ref, sems,
    grid=0.0, fine=0, start=0,
):
    copies = fetch(
        (widths_in, amps_in, delays_in, phases_in, chirps_in, prior_in),
        (widths_ref, amps_ref, delays_ref, phases_ref, chirps_ref, prior_ref),
        sems,
    )
    copies[0].wait()
    wide, upper = edges(widths_ref[...])
    bins = wide.shape[1]
    draws = features_ref.shape[2]
    mine = pl.ds(pl.multiple_of(lax.axis_index("bin") * draws, draws), draws)
    member = lax.broadcasted_iota(jnp.int32, place_ref.shape, 0)
    source = (member + start) % place_ref.shape[0] * fine
    passed = jnp.sum(jnp.where(upper <= source.astype(F32), 1, 0), axis=1, keepdims=True)
    place_ref[...] = jnp.broadcast_to((passed + (bins - 1)) % bins, place_ref.shape)
    step = upper * (TIME_STEP / grid)
    near = lax.broadcasted_iota(jnp.int32, (CHUNK, bins), 0).astype(F32)
    near_cos, near_sin = turn(near * step)
    for first in range(0, TSHIFT // 2 + TAIL, CHUNK):
        size = min(CHUNK, TSHIFT // 2 + TAIL - first)
        rows = slice(first, first + size)
        far_cos, far_sin = turn(float(first) * step)
        here_cos, here_sin = near_cos[:size], near_sin[:size]
        cosine = here_cos * far_cos - here_sin * far_sin
        sine = here_sin * far_cos + here_cos * far_sin
        cos_ref[rows, :bins], cos_ref[rows, bins:] = split(cosine)
        sin_ref[rows, :bins], sin_ref[rows, bins:] = split(sine)
    tall = jnp.concatenate([upper, jnp.zeros((bins - 1, bins), F32)], axis=0).T
    x = tall[:, :1] * (1.0 / grid)
    for copy in copies[1:]:
        copy.wait()
    chirps = chirps_ref[:, mine]
    base = phases_ref[:, mine] * (0.5 / math.pi)
    common = base + (chirps * (0.5 / math.pi)) * (x * x)
    cos0, sin0 = turn(base)
    for d in range(DET):
        amp = jnp.exp(amps_ref[d : d + 1, mine])
        delay = delays_ref[d : d + 1, mine]
        cosine, sine = turn(x * delay + common)
        features_ref[2 * d] = amp * cosine
        features_ref[2 * d + 1] = amp * sine
        flat_ref[2 * d : 2 * d + 1] = amp * cos0
        flat_ref[2 * d + 1 : 2 * d + 2] = amp * sin0
    flat_ref[6:7] = prior_ref[:, mine]
    flat_ref[7:8] = chirps
    flat_ref[8 : 8 + DET] = delays_ref[:, mine]
    flat_ref[8 + DET :] = jnp.zeros((8 - DET, draws), F32)


def score_kernel(
    sums_ref, cos_ref, sin_ref, features_ref, flat_ref, place_ref, out_ref, zero=0,
):
    bins = features_ref.shape[1]
    draws = features_ref.shape[2]
    half = TSHIFT // 2
    place = place_ref[...]
    row = lax.broadcasted_iota(jnp.int32, place.shape, 0)
    lane = lax.broadcasted_iota(jnp.int32, place.shape, 1)
    tiles = [sums_ref[:, 0, r * bins : (r + 1) * bins] for r in range(3)]
    last = sums_ref[:, 0, 3 * bins : PAYLOAD]
    rest = jnp.zeros((last.shape[0], 4 * bins - PAYLOAD), F32)
    tiles.append(jnp.concatenate([last, rest], axis=1))
    lines, single = [], []
    for c in range(CHANNELS):
        tile, off = divmod(c * SPAN, bins)
        line = pltpu.roll(tiles[tile], bins - off, 1) if off else tiles[tile]
        if off + SPAN > bins:
            line = jnp.where(lane < bins - off, line, pltpu.roll(tiles[tile + 1], bins - off, 1))
        line = shifted(jnp.where(lane < SPAN, line, 0.0), place)
        single.append(line[zero : zero + 1, bins - 1 :])
        line = jnp.where((row == zero) & (lane == bins - 1), 0.0, line)
        lines.append(jnp.sum(line, axis=0, keepdims=True))
    tall = jnp.concatenate(lines + [jnp.zeros((bins - CHANNELS, bins), F32)], axis=0).T
    extra = jnp.sum(tiles[3], axis=0, keepdims=True)
    extra = [
        pltpu.roll(extra, bins - CHANNELS * SPAN % bins - d * TERMS, 1) for d in range(DET)
    ]
    extra = jnp.concatenate(extra + [jnp.zeros((8 - DET, bins), F32)], axis=0)
    chirp = powers(jnp.broadcast_to(flat_ref[7:8], (8, draws)), 6)
    delay = powers(flat_ref[8:], 6)
    power = jnp.broadcast_to(extra[:, TERMS - 1 : TERMS], (8, draws))
    for k, (_, i, j) in enumerate(series()):
        power = power + extra[:, k : k + 1] * monomial(delay, chirp, i, j)
    real = imag = None
    offset = flat_ref[6:7]
    for d in range(DET):
        a, b = tall[:, 2 * d : 2 * d + 1], tall[:, 2 * d + 1 : 2 * d + 2]
        cosine, sine = features_ref[2 * d], features_ref[2 * d + 1]
        re, im = a * cosine + b * sine, b * cosine - a * sine
        real = re if real is None else real + re
        imag = im if imag is None else imag + im
        cos0, sin0 = flat_ref[2 * d : 2 * d + 1], flat_ref[2 * d + 1 : 2 * d + 2]
        offset = offset + single[2 * d] * cos0 + single[2 * d + 1] * sin0
        offset = offset - (0.5 * power[d : d + 1]) * (cos0 * cos0 + sin0 * sin0)
    real, imag = (
        [jnp.concatenate([piece, piece], axis=0) for piece in split(part * (1.0 / LOG2))]
        for part in (real, imag)
    )

    def rotated(rows, columns):
        return (
            jnp.dot(ref[rows, :], part[0][:, columns], preferred_element_type=F32)
            + jnp.dot(ref[rows, :], part[1][:, columns], preferred_element_type=F32)
            for ref, part in ((cos_ref, real), (sin_ref, imag))
        )

    marginal = []
    for start in range(0, draws, WIDE):
        columns = slice(start, start + WIDE)
        even, odd = rotated(slice(half, half + TAIL), columns)
        earliest = (even - odd)[:1]
        top = total = None
        for first in range(0, half, STRIP):
            even, odd = rotated(slice(first, first + STRIP), columns)
            after, before = even + odd, even - odd
            if first == 0:
                at = lax.broadcasted_iota(jnp.int32, before.shape, 0)
                before = jnp.where(at == 0, earliest, before)
            after = after.reshape(STRIP // 8, 8, WIDE)
            before = before.reshape(STRIP // 8, 8, WIDE)
            peak = jnp.max(jnp.maximum(after, before), axis=0)
            if top is not None:
                peak = jnp.maximum(peak, top)
                total = total * jnp.exp2(top - peak)
            add = jnp.sum(jnp.exp2(after - peak[None]) + jnp.exp2(before - peak[None]), axis=0)
            total = add if total is None else total + add
            top = peak
        peak = jnp.max(top, axis=0, keepdims=True)
        total = jnp.sum(total * jnp.exp2(top - peak), axis=0, keepdims=True)
        marginal.append(peak * LOG2 + (jnp.log(total) - math.log(TSHIFT)))
    marginal = jnp.concatenate(marginal, axis=1) + offset
    out_ref[...] = marginal[None]


def merged(stats):
    best, mass = stats[:, :, :1], stats[:, :, 1:2]
    top = jnp.max(best, axis=0, keepdims=True)
    return top, jnp.sum(mass * jnp.exp(best - top), axis=0, keepdims=True)


def stats_kernel(marginal_ref, out_ref):
    marginal = marginal_ref[...]
    best = jnp.max(jnp.max(marginal, axis=0, keepdims=True), axis=2, keepdims=True)
    mass = jnp.sum(jnp.exp(marginal - best), axis=0, keepdims=True)
    mass = jnp.sum(mass, axis=2, keepdims=True)
    lane = lax.broadcasted_iota(jnp.int32, (1, 1, LANES), 2)
    out_ref[...] = jnp.broadcast_to(jnp.where(lane == 0, best, mass), out_ref.shape)


def final_kernel(stats_ref, marginal_ref, out_ref, evidence_ref, draws=0):
    top, mass = merged(stats_ref[...])
    total = top + jnp.log(mass)
    out_ref[...] = marginal_ref[...] - total
    evidence_ref[...] = total[0] - math.log(draws)


def body(fine_cross, fine_power, bin_widths, log_amps, delays, phases, chirps, proposal_log):
    shards, cores = lax.axis_size("draw"), lax.axis_size("bin")
    detectors, fine = fine_power.shape
    bins = bin_widths.shape[0]
    whole = log_amps.shape[1]
    draws = whole // cores
    widths = bin_widths.reshape(1, bins)
    turned = [(i + int(shards * MEET)) % shards for i in range(shards)]
    args = (fine_cross, fine_power, widths)
    sums = call(
        functools.partial(summary_kernel, grid=float(fine * shards)),
        jax.ShapeDtypeStruct((shards, 1, PAYLOAD), F32),
        *args, scratch=landing(args), pinned=True, flops=1 << 24, name="summary",
    )
    everyone = lax.all_to_all(sums, "draw", 0, 0, axis_index_groups=[turned], tiled=True)
    args = (
        widths, log_amps, delays, phases.reshape(1, whole), chirps.reshape(1, whole),
        proposal_log.reshape(1, whole),
    )
    terms = call(
        functools.partial(terms_kernel, grid=float(fine * shards), fine=fine, start=turned[0]),
        (
            jax.ShapeDtypeStruct((TSHIFT // 2 + TAIL, 2 * bins), BF16),
            jax.ShapeDtypeStruct((TSHIFT // 2 + TAIL, 2 * bins), BF16),
            jax.ShapeDtypeStruct((2 * detectors, bins, draws), F32),
            jax.ShapeDtypeStruct((16, draws), F32),
            jax.ShapeDtypeStruct((shards, bins), jnp.int32),
        ),
        *args, scratch=landing(args), pinned=True, flops=1 << 28, name="terms",
    )
    marginal = call(
        functools.partial(score_kernel, zero=turned.index(0)),
        jax.ShapeDtypeStruct((1, 1, draws), F32),
        everyone, *terms, flops=1 << 30, name="score",
    )
    marginals = lax.all_gather(marginal, "bin", axis=0, tiled=True)
    stat = call(
        stats_kernel, jax.ShapeDtypeStruct((shards, 1, LANES), F32), marginals, name="stats"
    )
    stats = lax.all_to_all(stat, "draw", 0, 0, axis_index_groups=[turned], tiled=True)
    weights, evidence = call(
        lambda *refs: final_kernel(*refs, draws=whole * shards),
        (
            jax.ShapeDtypeStruct((cores, 1, draws), F32),
            jax.ShapeDtypeStruct((1, 1), F32),
        ),
        stats, marginals, name="final",
    )
    return weights.reshape(whole), evidence.reshape(1)


def solution(mesh):
    placed = (
        P("event", None, "draw"),
        P("event", "draw"),
        P("event"),
        P("event", "draw"),
        P("event", "draw"),
        P(("event", "draw")),
        P(("event", "draw")),
        P(("event", "draw")),
    )
    return jax.shard_map(
        body,
        mesh=mesh,
        in_specs=placed,
        out_specs=(P(("event", "draw")), P("event")),
        check_vma=False,
    )
```

```python
import functools
import math

import jax
import jax.numpy as jnp
import numpy as np
from jax import lax
from jax.experimental import pallas as pl
from jax.experimental.pallas import tpu as pltpu
from jax.sharding import PartitionSpec as P

TSHIFT = 2048
TIME_STEP = 0.125
LOG2 = math.log(2.0)
WIDE = 256
CHUNK = 128
TAIL = 16
STRIP = 32
LONG = 512
LANES = 128
DET = 3
CHANNELS = 6
SPAN = 68
TERMS = 16
PAYLOAD = CHANNELS * SPAN + DET * TERMS
MEET = 0.75
VMEM = pl.BlockSpec(memory_space=pltpu.VMEM)
F32, BF16 = jnp.float32, jnp.bfloat16


def fit(function, terms):
    nodes = 0.125 * (1.0 + np.cos((np.arange(64) + 0.5) * np.pi / 64))
    basis = np.vander(nodes / 0.25, terms, increasing=True)
    found = np.linalg.lstsq(basis, function(np.sqrt(nodes)), rcond=None)[0]
    return [float(c) for c in found / 0.25 ** np.arange(terms)]


COS = fit(lambda r: np.cos(np.pi * r), 7)
SIN = fit(lambda r: np.sin(np.pi * r) / r, 6)


def horner(coefficients, x):
    total = jnp.full_like(x, coefficients[-1])
    for c in coefficients[-2::-1]:
        total = total * x + c
    return total


def turn(u):
    r = u - jnp.round(u)
    square = r * r
    cosine, sine = horner(COS, square), horner(SIN, square) * r
    twice = sine + sine
    return 1.0 - twice * sine, twice * cosine


def call(kernel, outs, *args, scratch=(), pinned=False, limit=24 << 20, flops=1 << 20, name=None):
    where = VMEM
    if pinned:
        where = pl.BlockSpec(memory_space=pltpu.HBM)
        args = [pltpu.with_memory_space_constraint(a, pltpu.HBM) for a in args]
    return pl.pallas_call(
        kernel,
        out_shape=outs,
        in_specs=[where] * len(args),
        out_specs=jax.tree.map(lambda _: VMEM, outs),
        scratch_shapes=scratch,
        compiler_params=pltpu.CompilerParams(vmem_limit_bytes=limit),
        cost_estimate=pl.CostEstimate(flops=flops, bytes_accessed=1 << 20, transcendentals=0),
        name=name,
    )(*args)


def landing(args):
    return [pltpu.VMEM(a.shape, a.dtype) for a in args] + [pltpu.SemaphoreType.DMA((len(args),))]


def fetch(sources, targets, semaphores):
    copies = [
        pltpu.make_async_copy(source, target, semaphores.at[i])
        for i, (source, target) in enumerate(zip(sources, targets))
    ]
    for copy in copies:
        copy.start()
    return copies


def shifted(x, amount):
    for bit in range(LANES.bit_length() - 1):
        x = jnp.where((amount >> bit) & 1 == 1, pltpu.roll(x, 1 << bit, 1), x)
    return x


def series():
    return [
        (-4.0 * c * math.comb(n, j), n - j, j)
        for n, c in ((2, 1.0), (4, -1.0 / 3), (6, 2.0 / 45))
        for j in range(n + 1)
    ]


def powers(x, count):
    found = [None, x]
    while len(found) <= count:
        found.append(found[-1] * x)
    return found


def monomial(left, right, i, j):
    if i and j:
        return left[i] * right[j]
    return left[i] if i else right[j]


def edges(widths):
    wide = widths.astype(F32)
    bins = wide.shape[1]
    before = lax.broadcasted_iota(jnp.int32, (bins, bins), 0)
    mine = lax.broadcasted_iota(jnp.int32, (bins, bins), 1)
    ones = jnp.where(before <= mine, 1.0, 0.0).astype(BF16)
    rows = jnp.broadcast_to(wide, (16, bins)).astype(BF16)
    upper = jnp.dot(rows, ones, preferred_element_type=F32)[:1]
    return wide, upper


def split(x):
    high = x.astype(BF16)
    return high, (x - high.astype(F32)).astype(BF16)


def summary_kernel(
    cross_in, power_in, widths_in, out_ref, cross_ref, power_ref, widths_ref, sems, grid=0.0
):
    for copy in fetch(
        (widths_in, cross_in, power_in), (widths_ref, cross_ref, power_ref), sems
    ):
        copy.wait()
    fine, bins = power_ref.shape[1], widths_ref.shape[1]
    wide, upper = edges(widths_ref[...])
    lower = upper - wide
    first = (lax.axis_index("draw") * fine).astype(F32)
    at = lax.broadcasted_iota(jnp.int32, (fine, bins), 0).astype(F32) + first
    inside = (at >= lower) & (at < upper)
    up = jnp.where(inside, 2.0 * (at - lower) + 1.0, 0.0)
    down = jnp.where(inside, 2.0 * wide - up, 0.0)
    both_high, both_low = split(up * down)
    weights = jnp.concatenate([up.astype(BF16), down.astype(BF16), both_high, both_low], axis=1)
    data = jnp.concatenate(
        [cross_ref[d] for d in range(DET)] + [power_ref[...], jnp.zeros((7, fine), F32)], axis=0
    )
    high = data.astype(BF16)
    rest = data - high.astype(F32)
    middle, low = split(rest)
    got = jnp.dot(
        jnp.concatenate([high, middle, low], axis=0), weights, preferred_element_type=F32
    )
    got = got[:16] + got[16:32] + got[32:]
    scale = 0.5 / wide
    end = got[:, :bins] * scale
    start = got[:, bins : 2 * bins] * scale
    mixed = (got[:, 2 * bins : 3 * bins] + got[:, 3 * bins :]) * (scale * scale)
    row = lax.broadcasted_iota(jnp.int32, (16, bins), 0)
    lane = lax.broadcasted_iota(jnp.int32, (16, bins), 1)
    merged = end + pltpu.roll(start, bins - 1, 1)
    passed = jnp.sum(jnp.where(upper <= first, 1, 0), axis=1, keepdims=True)
    table = shifted(merged, (bins + 1 - passed) % bins)
    width, x = wide * (1.0 / grid), upper * (1.0 / grid)
    slope = powers(math.pi * width, 6)
    bend = powers(0.5 * width * (x + (x - width)), 6)
    factors = [c * monomial(slope, bend, i, j) for c, i, j in series()]
    factors = jnp.concatenate(factors + [jnp.zeros((1, bins), F32)], axis=0)
    extra = jnp.zeros((TERMS, bins), F32)
    total = jnp.sum(data, axis=1, keepdims=True)
    for d in range(DET):
        each = jnp.sum(factors * mixed[6 + d : 7 + d], axis=1, keepdims=True)
        each = jnp.where(row[:, :1] == TERMS - 1, total[6 + d : 7 + d], each)
        extra = jnp.where(lane == row + (CHANNELS * SPAN % bins + d * TERMS), each, extra)
    tiles = [jnp.zeros((1, bins), F32)] * 4
    tiles[3] = jnp.sum(extra, axis=0, keepdims=True)
    lane = lane[:1]
    for c in range(CHANNELS):
        tile, off = divmod(c * SPAN, bins)
        line = pltpu.roll(table[c : c + 1], off, 1) if off else table[c : c + 1]
        tiles[tile] = tiles[tile] + jnp.where(lane >= off, line, 0.0)
        if off + SPAN > bins:
            tiles[tile + 1] = tiles[tile + 1] + jnp.where(lane < off, line, 0.0)
    for r, tile in enumerate(tiles):
        end = min((r + 1) * bins, PAYLOAD)
        out_ref[:, :, r * bins : end] = jnp.broadcast_to(
            tile[None, :, : end - r * bins], (out_ref.shape[0], 1, end - r * bins)
        )


def terms_kernel(
    widths_in, amps_in, delays_in, phases_in, chirps_in, prior_in,
    cos_ref, sin_ref, features_ref, flat_ref, place_ref,
    widths_ref, amps_ref, delays_ref, phases_ref, chirps_ref, prior_ref, sems,
    grid=0.0, fine=0, start=0,
):
    copies = fetch(
        (widths_in, amps_in, delays_in, phases_in, chirps_in, prior_in),
        (widths_ref, amps_ref, delays_ref, phases_ref, chirps_ref, prior_ref),
        sems,
    )
    copies[0].wait()
    wide, upper = edges(widths_ref[...])
    bins = wide.shape[1]
    draws = features_ref.shape[2]
    mine = pl.ds(pl.multiple_of(lax.axis_index("bin") * draws, draws), draws)
    member = lax.broadcasted_iota(jnp.int32, place_ref.shape, 0)
    source = (member + start) % place_ref.shape[0] * fine
    passed = jnp.sum(jnp.where(upper <= source.astype(F32), 1, 0), axis=1, keepdims=True)
    place_ref[...] = jnp.broadcast_to((passed + (bins - 1)) % bins, place_ref.shape)
    step = upper * (TIME_STEP / grid)
    near = lax.broadcasted_iota(jnp.int32, (CHUNK, bins), 0).astype(F32)
    near_cos, near_sin = turn(near * step)
    for first in range(0, TSHIFT // 2 + TAIL, CHUNK):
        size = min(CHUNK, TSHIFT // 2 + TAIL - first)
        rows = slice(first, first + size)
        far_cos, far_sin = turn(float(first) * step)
        here_cos, here_sin = near_cos[:size], near_sin[:size]
        cosine = here_cos * far_cos - here_sin * far_sin
        sine = here_sin * far_cos + here_cos * far_sin
        cos_ref[rows, :bins], cos_ref[rows, bins:] = split(cosine)
        sin_ref[rows, :bins], sin_ref[rows, bins:] = split(sine)
    tall = jnp.concatenate([upper, jnp.zeros((bins - 1, bins), F32)], axis=0).T
    x = tall[:, :1] * (1.0 / grid)
    for copy in copies[1:]:
        copy.wait()
    chirps = chirps_ref[:, mine]
    base = phases_ref[:, mine] * (0.5 / math.pi)
    common = base + (chirps * (0.5 / math.pi)) * (x * x)
    cos0, sin0 = turn(base)
    for d in range(DET):
        amp = jnp.exp(amps_ref[d : d + 1, mine])
        delay = delays_ref[d : d + 1, mine]
        cosine, sine = turn(x * delay + common)
        features_ref[2 * d] = amp * cosine
        features_ref[2 * d + 1] = amp * sine
        flat_ref[2 * d : 2 * d + 1] = amp * cos0
        flat_ref[2 * d + 1 : 2 * d + 2] = amp * sin0
    flat_ref[6:7] = prior_ref[:, mine]
    flat_ref[7:8] = chirps
    flat_ref[8 : 8 + DET] = delays_ref[:, mine]
    flat_ref[8 + DET :] = jnp.zeros((8 - DET, draws), F32)


def score_kernel(
    sums_ref, cos_ref, sin_ref, features_ref, flat_ref, place_ref, out_ref,
    even_ref, odd_ref, zero=0,
):
    bins = features_ref.shape[1]
    draws = features_ref.shape[2]
    half = TSHIFT // 2
    place = place_ref[...]
    row = lax.broadcasted_iota(jnp.int32, place.shape, 0)
    lane = lax.broadcasted_iota(jnp.int32, place.shape, 1)
    tiles = [sums_ref[:, 0, r * bins : (r + 1) * bins] for r in range(3)]
    last = sums_ref[:, 0, 3 * bins : PAYLOAD]
    rest = jnp.zeros((last.shape[0], 4 * bins - PAYLOAD), F32)
    tiles.append(jnp.concatenate([last, rest], axis=1))
    lines, single = [], []
    for c in range(CHANNELS):
        tile, off = divmod(c * SPAN, bins)
        line = pltpu.roll(tiles[tile], bins - off, 1) if off else tiles[tile]
        if off + SPAN > bins:
            line = jnp.where(lane < bins - off, line, pltpu.roll(tiles[tile + 1], bins - off, 1))
        line = shifted(jnp.where(lane < SPAN, line, 0.0), place)
        single.append(line[zero : zero + 1, bins - 1 :])
        line = jnp.where((row == zero) & (lane == bins - 1), 0.0, line)
        lines.append(jnp.sum(line, axis=0, keepdims=True))
    tall = jnp.concatenate(lines + [jnp.zeros((bins - CHANNELS, bins), F32)], axis=0).T
    extra = jnp.sum(tiles[3], axis=0, keepdims=True)
    extra = [
        pltpu.roll(extra, bins - CHANNELS * SPAN % bins - d * TERMS, 1) for d in range(DET)
    ]
    extra = jnp.concatenate(extra + [jnp.zeros((8 - DET, bins), F32)], axis=0)
    chirp = powers(jnp.broadcast_to(flat_ref[7:8], (8, draws)), 6)
    delay = powers(flat_ref[8:], 6)
    power = jnp.broadcast_to(extra[:, TERMS - 1 : TERMS], (8, draws))
    for k, (_, i, j) in enumerate(series()):
        power = power + extra[:, k : k + 1] * monomial(delay, chirp, i, j)
    real = imag = None
    offset = flat_ref[6:7]
    for d in range(DET):
        a, b = tall[:, 2 * d : 2 * d + 1], tall[:, 2 * d + 1 : 2 * d + 2]
        cosine, sine = features_ref[2 * d], features_ref[2 * d + 1]
        re, im = a * cosine + b * sine, b * cosine - a * sine
        real = re if real is None else real + re
        imag = im if imag is None else imag + im
        cos0, sin0 = flat_ref[2 * d : 2 * d + 1], flat_ref[2 * d + 1 : 2 * d + 2]
        offset = offset + single[2 * d] * cos0 + single[2 * d + 1] * sin0
        offset = offset - (0.5 * power[d : d + 1]) * (cos0 * cos0 + sin0 * sin0)
    real, imag = (
        [jnp.concatenate([piece, piece], axis=0) for piece in split(part * (1.0 / LOG2))]
        for part in (real, imag)
    )

    def rotated(rows, columns):
        return (
            jnp.dot(ref[rows, :], part[0][:, columns], preferred_element_type=F32)
            + jnp.dot(ref[rows, :], part[1][:, columns], preferred_element_type=F32)
            for ref, part in ((cos_ref, real), (sin_ref, imag))
        )

    marginal = []
    for start in range(0, draws, WIDE):
        columns = slice(start, start + WIDE)
        even, odd = rotated(slice(half, half + TAIL), columns)
        earliest = (even - odd)[:1]
        top = total = None
        for first in range(0, half, STRIP):
            if first % LONG == 0:
                rows = slice(first, first + LONG)
                even_ref[rows, columns], odd_ref[rows, columns] = rotated(rows, columns)
            rows = slice(first, first + STRIP)
            even, odd = even_ref[rows, columns], odd_ref[rows, columns]
            after, before = even + odd, even - odd
            if first == 0:
                at = lax.broadcasted_iota(jnp.int32, before.shape, 0)
                before = jnp.where(at == 0, earliest, before)
            after = after.reshape(STRIP // 8, 8, WIDE)
            before = before.reshape(STRIP // 8, 8, WIDE)
            peak = jnp.max(jnp.maximum(after, before), axis=0)
            if top is not None:
                peak = jnp.maximum(peak, top)
                total = total * jnp.exp2(top - peak)
            add = jnp.sum(jnp.exp2(after - peak[None]) + jnp.exp2(before - peak[None]), axis=0)
            total = add if total is None else total + add
            top = peak
        peak = jnp.max(top, axis=0, keepdims=True)
        total = jnp.sum(total * jnp.exp2(top - peak), axis=0, keepdims=True)
        marginal.append(peak * LOG2 + (jnp.log(total) - math.log(TSHIFT)))
    marginal = jnp.concatenate(marginal, axis=1) + offset
    out_ref[...] = marginal[None]


def merged(stats):
    best, mass = stats[:, :, :1], stats[:, :, 1:2]
    top = jnp.max(best, axis=0, keepdims=True)
    return top, jnp.sum(mass * jnp.exp(best - top), axis=0, keepdims=True)


def stats_kernel(marginal_ref, out_ref):
    marginal = marginal_ref[...]
    best = jnp.max(jnp.max(marginal, axis=0, keepdims=True), axis=2, keepdims=True)
    mass = jnp.sum(jnp.exp(marginal - best), axis=0, keepdims=True)
    mass = jnp.sum(mass, axis=2, keepdims=True)
    lane = lax.broadcasted_iota(jnp.int32, (1, 1, LANES), 2)
    out_ref[...] = jnp.broadcast_to(jnp.where(lane == 0, best, mass), out_ref.shape)


def final_kernel(stats_ref, marginal_ref, out_ref, evidence_ref, draws=0):
    top, mass = merged(stats_ref[...])
    total = top + jnp.log(mass)
    out_ref[...] = marginal_ref[...] - total
    evidence_ref[...] = total[0] - math.log(draws)


def body(fine_cross, fine_power, bin_widths, log_amps, delays, phases, chirps, proposal_log):
    shards, cores = lax.axis_size("draw"), lax.axis_size("bin")
    detectors, fine = fine_power.shape
    bins = bin_widths.shape[0]
    whole = log_amps.shape[1]
    draws = whole // cores
    widths = bin_widths.reshape(1, bins)
    turned = [(i + int(shards * MEET)) % shards for i in range(shards)]
    args = (fine_cross, fine_power, widths)
    sums = call(
        functools.partial(summary_kernel, grid=float(fine * shards)),
        jax.ShapeDtypeStruct((shards, 1, PAYLOAD), F32),
        *args, scratch=landing(args), pinned=True, flops=1 << 24, name="summary",
    )
    everyone = lax.all_to_all(sums, "draw", 0, 0, axis_index_groups=[turned], tiled=True)
    args = (
        widths, log_amps, delays, phases.reshape(1, whole), chirps.reshape(1, whole),
        proposal_log.reshape(1, whole),
    )
    terms = call(
        functools.partial(terms_kernel, grid=float(fine * shards), fine=fine, start=turned[0]),
        (
            jax.ShapeDtypeStruct((TSHIFT // 2 + TAIL, 2 * bins), BF16),
            jax.ShapeDtypeStruct((TSHIFT // 2 + TAIL, 2 * bins), BF16),
            jax.ShapeDtypeStruct((2 * detectors, bins, draws), F32),
            jax.ShapeDtypeStruct((16, draws), F32),
            jax.ShapeDtypeStruct((shards, bins), jnp.int32),
        ),
        *args, scratch=landing(args), pinned=True, flops=1 << 28, name="terms",
    )
    marginal = call(
        functools.partial(score_kernel, zero=turned.index(0)),
        jax.ShapeDtypeStruct((1, 1, draws), F32),
        everyone, *terms, scratch=[pltpu.VMEM((TSHIFT // 2, draws), F32)] * 2, flops=1 << 30, name="score",
    )
    marginals = lax.all_gather(marginal, "bin", axis=0, tiled=True)
    stat = call(
        stats_kernel, jax.ShapeDtypeStruct((shards, 1, LANES), F32), marginals, name="stats"
    )
    stats = lax.all_to_all(stat, "draw", 0, 0, axis_index_groups=[turned], tiled=True)
    weights, evidence = call(
        lambda *refs: final_kernel(*refs, draws=whole * shards),
        (
            jax.ShapeDtypeStruct((cores, 1, draws), F32),
            jax.ShapeDtypeStruct((1, 1), F32),
        ),
        stats, marginals, name="final",
    )
    return weights.reshape(whole), evidence.reshape(1)


def solution(mesh):
    placed = (
        P("event", None, "draw"),
        P("event", "draw"),
        P("event"),
        P("event", "draw"),
        P("event", "draw"),
        P(("event", "draw")),
        P(("event", "draw")),
        P(("event", "draw")),
    )
    return jax.shard_map(
        body,
        mesh=mesh,
        in_specs=placed,
        out_specs=(P(("event", "draw")), P("event")),
        check_vma=False,
    )
```

```python
import functools
import math

import jax
import jax.numpy as jnp
import numpy as np
from jax import lax
from jax.experimental import pallas as pl
from jax.experimental.pallas import tpu as pltpu
from jax.sharding import PartitionSpec as P

TSHIFT = 2048
TIME_STEP = 0.125
LOG2 = math.log(2.0)
WIDE = 256
CHUNK = 128
TAIL = 16
STRIP = 128
LANES = 128
DET = 3
CHANNELS = 6
SPAN = 68
TERMS = 16
PAYLOAD = CHANNELS * SPAN + DET * TERMS
MEET = (0.75, 0.5)
VMEM = pl.BlockSpec(memory_space=pltpu.VMEM)
F32, BF16 = jnp.float32, jnp.bfloat16


def fit(function, terms):
    nodes = 0.125 * (1.0 + np.cos((np.arange(64) + 0.5) * np.pi / 64))
    basis = np.vander(nodes / 0.25, terms, increasing=True)
    found = np.linalg.lstsq(basis, function(np.sqrt(nodes)), rcond=None)[0]
    return [float(c) for c in found / 0.25 ** np.arange(terms)]


COS = fit(lambda r: np.cos(np.pi * r), 7)
SIN = fit(lambda r: np.sin(np.pi * r) / r, 6)


def horner(coefficients, x):
    total = jnp.full_like(x, coefficients[-1])
    for c in coefficients[-2::-1]:
        total = total * x + c
    return total


def turn(u):
    r = u - jnp.round(u)
    square = r * r
    cosine, sine = horner(COS, square), horner(SIN, square) * r
    twice = sine + sine
    return 1.0 - twice * sine, twice * cosine


def call(kernel, outs, *args, scratch=(), pinned=False, limit=24 << 20, flops=1 << 20, name=None):
    where = VMEM
    if pinned:
        where = pl.BlockSpec(memory_space=pltpu.HBM)
        args = [pltpu.with_memory_space_constraint(a, pltpu.HBM) for a in args]
    return pl.pallas_call(
        kernel,
        out_shape=outs,
        in_specs=[where] * len(args),
        out_specs=jax.tree.map(lambda _: VMEM, outs),
        scratch_shapes=scratch,
        compiler_params=pltpu.CompilerParams(vmem_limit_bytes=limit),
        cost_estimate=pl.CostEstimate(flops=flops, bytes_accessed=1 << 20, transcendentals=0),
        name=name,
    )(*args)


def landing(args):
    return [pltpu.VMEM(a.shape, a.dtype) for a in args] + [pltpu.SemaphoreType.DMA((len(args),))]


def fetch(sources, targets, semaphores):
    copies = [
        pltpu.make_async_copy(source, target, semaphores.at[i])
        for i, (source, target) in enumerate(zip(sources, targets))
    ]
    for copy in copies:
        copy.start()
    return copies


def shifted(x, amount):
    for bit in range(LANES.bit_length() - 1):
        x = jnp.where((amount >> bit) & 1 == 1, pltpu.roll(x, 1 << bit, 1), x)
    return x


def series():
    return [
        (-4.0 * c * math.comb(n, j), n - j, j)
        for n, c in ((2, 1.0), (4, -1.0 / 3), (6, 2.0 / 45))
        for j in range(n + 1)
    ]


def powers(x, count):
    found = [None, x]
    while len(found) <= count:
        found.append(found[-1] * x)
    return found


def monomial(left, right, i, j):
    if i and j:
        return left[i] * right[j]
    return left[i] if i else right[j]


def edges(widths):
    wide = widths.astype(F32)
    bins = wide.shape[1]
    before = lax.broadcasted_iota(jnp.int32, (bins, bins), 0)
    mine = lax.broadcasted_iota(jnp.int32, (bins, bins), 1)
    ones = jnp.where(before <= mine, 1.0, 0.0).astype(BF16)
    rows = jnp.broadcast_to(wide, (16, bins)).astype(BF16)
    upper = jnp.dot(rows, ones, preferred_element_type=F32)[:1]
    return wide, upper


def split(x):
    high = x.astype(BF16)
    return high, (x - high.astype(F32)).astype(BF16)


def summary_kernel(
    cross_in, power_in, widths_in, out_ref, cross_ref, power_ref, widths_ref, sems, grid=0.0
):
    for copy in fetch(
        (widths_in, cross_in, power_in), (widths_ref, cross_ref, power_ref), sems
    ):
        copy.wait()
    fine, bins = power_ref.shape[1], widths_ref.shape[1]
    wide, upper = edges(widths_ref[...])
    lower = upper - wide
    first = (lax.axis_index("draw") * fine).astype(F32)
    at = lax.broadcasted_iota(jnp.int32, (fine, bins), 0).astype(F32) + first
    inside = (at >= lower) & (at < upper)
    up = jnp.where(inside, 2.0 * (at - lower) + 1.0, 0.0)
    down = jnp.where(inside, 2.0 * wide - up, 0.0)
    both_high, both_low = split(up * down)
    weights = jnp.concatenate([up.astype(BF16), down.astype(BF16), both_high, both_low], axis=1)
    data = jnp.concatenate(
        [cross_ref[d] for d in range(DET)] + [power_ref[...], jnp.zeros((7, fine), F32)], axis=0
    )
    high = data.astype(BF16)
    rest = data - high.astype(F32)
    middle, low = split(rest)
    got = jnp.dot(
        jnp.concatenate([high, middle, low], axis=0), weights, preferred_element_type=F32
    )
    got = got[:16] + got[16:32] + got[32:]
    scale = 0.5 / wide
    end = got[:, :bins] * scale
    start = got[:, bins : 2 * bins] * scale
    mixed = (got[:, 2 * bins : 3 * bins] + got[:, 3 * bins :]) * (scale * scale)
    row = lax.broadcasted_iota(jnp.int32, (16, bins), 0)
    lane = lax.broadcasted_iota(jnp.int32, (16, bins), 1)
    merged = end + pltpu.roll(start, bins - 1, 1)
    passed = jnp.sum(jnp.where(upper <= first, 1, 0), axis=1, keepdims=True)
    table = shifted(merged, (bins + 1 - passed) % bins)
    width, x = wide * (1.0 / grid), upper * (1.0 / grid)
    slope = powers(math.pi * width, 6)
    bend = powers(0.5 * width * (x + (x - width)), 6)
    factors = [c * monomial(slope, bend, i, j) for c, i, j in series()]
    factors = jnp.concatenate(factors + [jnp.zeros((1, bins), F32)], axis=0)
    extra = jnp.zeros((TERMS, bins), F32)
    total = jnp.sum(data, axis=1, keepdims=True)
    for d in range(DET):
        each = jnp.sum(factors * mixed[6 + d : 7 + d], axis=1, keepdims=True)
        each = jnp.where(row[:, :1] == TERMS - 1, total[6 + d : 7 + d], each)
        extra = jnp.where(lane == row + (CHANNELS * SPAN % bins + d * TERMS), each, extra)
    tiles = [jnp.zeros((1, bins), F32)] * 4
    tiles[3] = jnp.sum(extra, axis=0, keepdims=True)
    lane = lane[:1]
    for c in range(CHANNELS):
        tile, off = divmod(c * SPAN, bins)
        line = pltpu.roll(table[c : c + 1], off, 1) if off else table[c : c + 1]
        tiles[tile] = tiles[tile] + jnp.where(lane >= off, line, 0.0)
        if off + SPAN > bins:
            tiles[tile + 1] = tiles[tile + 1] + jnp.where(lane < off, line, 0.0)
    for r, tile in enumerate(tiles):
        end = min((r + 1) * bins, PAYLOAD)
        out_ref[:, :, r * bins : end] = jnp.broadcast_to(
            tile[None, :, : end - r * bins], (out_ref.shape[0], 1, end - r * bins)
        )


def terms_kernel(
    widths_in, amps_in, delays_in, phases_in, chirps_in, prior_in,
    cos_ref, sin_ref, features_ref, flat_ref, place_ref,
    widths_ref, amps_ref, delays_ref, phases_ref, chirps_ref, prior_ref, sems,
    grid=0.0, fine=0, start=0,
):
    copies = fetch(
        (widths_in, amps_in, delays_in, phases_in, chirps_in, prior_in),
        (widths_ref, amps_ref, delays_ref, phases_ref, chirps_ref, prior_ref),
        sems,
    )
    copies[0].wait()
    wide, upper = edges(widths_ref[...])
    bins = wide.shape[1]
    draws = features_ref.shape[2]
    mine = pl.ds(pl.multiple_of(lax.axis_index("bin") * draws, draws), draws)
    member = lax.broadcasted_iota(jnp.int32, place_ref.shape, 0)
    source = (member + start) % place_ref.shape[0] * fine
    passed = jnp.sum(jnp.where(upper <= source.astype(F32), 1, 0), axis=1, keepdims=True)
    place_ref[...] = jnp.broadcast_to((passed + (bins - 1)) % bins, place_ref.shape)
    step = upper * (TIME_STEP / grid)
    near = lax.broadcasted_iota(jnp.int32, (CHUNK, bins), 0).astype(F32)
    near_cos, near_sin = turn(near * step)
    for first in range(0, TSHIFT // 2 + TAIL, CHUNK):
        size = min(CHUNK, TSHIFT // 2 + TAIL - first)
        rows = slice(first, first + size)
        far_cos, far_sin = turn(float(first) * step)
        here_cos, here_sin = near_cos[:size], near_sin[:size]
        cosine = here_cos * far_cos - here_sin * far_sin
        sine = here_sin * far_cos + here_cos * far_sin
        cos_ref[rows, :bins], cos_ref[rows, bins:] = split(cosine)
        sin_ref[rows, :bins], sin_ref[rows, bins:] = split(sine)
    tall = jnp.concatenate([upper, jnp.zeros((bins - 1, bins), F32)], axis=0).T
    x = tall[:, :1] * (1.0 / grid)
    for copy in copies[1:]:
        copy.wait()
    chirps = chirps_ref[:, mine]
    base = phases_ref[:, mine] * (0.5 / math.pi)
    common = base + (chirps * (0.5 / math.pi)) * (x * x)
    cos0, sin0 = turn(base)
    for d in range(DET):
        amp = jnp.exp(amps_ref[d : d + 1, mine])
        delay = delays_ref[d : d + 1, mine]
        cosine, sine = turn(x * delay + common)
        features_ref[2 * d] = amp * cosine
        features_ref[2 * d + 1] = amp * sine
        flat_ref[2 * d : 2 * d + 1] = amp * cos0
        flat_ref[2 * d + 1 : 2 * d + 2] = amp * sin0
    flat_ref[6:7] = prior_ref[:, mine]
    flat_ref[7:8] = chirps
    flat_ref[8 : 8 + DET] = delays_ref[:, mine]
    flat_ref[8 + DET :] = jnp.zeros((8 - DET, draws), F32)


def score_kernel(
    sums_ref, cos_ref, sin_ref, features_ref, flat_ref, place_ref, out_ref, zero=0,
):
    bins = features_ref.shape[1]
    draws = features_ref.shape[2]
    half = TSHIFT // 2
    place = place_ref[...]
    row = lax.broadcasted_iota(jnp.int32, place.shape, 0)
    lane = lax.broadcasted_iota(jnp.int32, place.shape, 1)
    tiles = [sums_ref[:, 0, r * bins : (r + 1) * bins] for r in range(3)]
    last = sums_ref[:, 0, 3 * bins : PAYLOAD]
    rest = jnp.zeros((last.shape[0], 4 * bins - PAYLOAD), F32)
    tiles.append(jnp.concatenate([last, rest], axis=1))
    lines, single = [], []
    for c in range(CHANNELS):
        tile, off = divmod(c * SPAN, bins)
        line = pltpu.roll(tiles[tile], bins - off, 1) if off else tiles[tile]
        if off + SPAN > bins:
            line = jnp.where(lane < bins - off, line, pltpu.roll(tiles[tile + 1], bins - off, 1))
        line = shifted(jnp.where(lane < SPAN, line, 0.0), place)
        single.append(line[zero : zero + 1, bins - 1 :])
        line = jnp.where((row == zero) & (lane == bins - 1), 0.0, line)
        lines.append(jnp.sum(line, axis=0, keepdims=True))
    tall = jnp.concatenate(lines + [jnp.zeros((bins - CHANNELS, bins), F32)], axis=0).T
    extra = jnp.sum(tiles[3], axis=0, keepdims=True)
    extra = [
        pltpu.roll(extra, bins - CHANNELS * SPAN % bins - d * TERMS, 1) for d in range(DET)
    ]
    extra = jnp.concatenate(extra + [jnp.zeros((8 - DET, bins), F32)], axis=0)
    chirp = powers(jnp.broadcast_to(flat_ref[7:8], (8, draws)), 6)
    delay = powers(flat_ref[8:], 6)
    power = jnp.broadcast_to(extra[:, TERMS - 1 : TERMS], (8, draws))
    for k, (_, i, j) in enumerate(series()):
        power = power + extra[:, k : k + 1] * monomial(delay, chirp, i, j)
    real = imag = None
    offset = flat_ref[6:7]
    for d in range(DET):
        a, b = tall[:, 2 * d : 2 * d + 1], tall[:, 2 * d + 1 : 2 * d + 2]
        cosine, sine = features_ref[2 * d], features_ref[2 * d + 1]
        re, im = a * cosine + b * sine, b * cosine - a * sine
        real = re if real is None else real + re
        imag = im if imag is None else imag + im
        cos0, sin0 = flat_ref[2 * d : 2 * d + 1], flat_ref[2 * d + 1 : 2 * d + 2]
        offset = offset + single[2 * d] * cos0 + single[2 * d + 1] * sin0
        offset = offset - (0.5 * power[d : d + 1]) * (cos0 * cos0 + sin0 * sin0)
    real, imag = (
        [jnp.concatenate([piece, piece], axis=0) for piece in split(part * (1.0 / LOG2))]
        for part in (real, imag)
    )

    def rotated(rows, columns):
        return (
            jnp.dot(ref[rows, :], part[0][:, columns], preferred_element_type=F32)
            + jnp.dot(ref[rows, :], part[1][:, columns], preferred_element_type=F32)
            for ref, part in ((cos_ref, real), (sin_ref, imag))
        )

    marginal = []
    for start in range(0, draws, WIDE):
        columns = slice(start, start + WIDE)
        even, odd = rotated(slice(half, half + TAIL), columns)
        earliest = (even - odd)[:1]
        top = total = None
        for first in range(0, half, STRIP):
            even, odd = rotated(slice(first, first + STRIP), columns)
            after, before = even + odd, even - odd
            if first == 0:
                at = lax.broadcasted_iota(jnp.int32, before.shape, 0)
                before = jnp.where(at == 0, earliest, before)
            after = after.reshape(STRIP // 8, 8, WIDE)
            before = before.reshape(STRIP // 8, 8, WIDE)
            peak = jnp.max(jnp.maximum(after, before), axis=0)
            if top is not None:
                peak = jnp.maximum(peak, top)
                total = total * jnp.exp2(top - peak)
            add = jnp.sum(jnp.exp2(after - peak[None]) + jnp.exp2(before - peak[None]), axis=0)
            total = add if total is None else total + add
            top = peak
        peak = jnp.max(top, axis=0, keepdims=True)
        total = jnp.sum(total * jnp.exp2(top - peak), axis=0, keepdims=True)
        marginal.append(peak * LOG2 + (jnp.log(total) - math.log(TSHIFT)))
    marginal = jnp.concatenate(marginal, axis=1) + offset
    out_ref[...] = marginal[None]


def merged(stats):
    best, mass = stats[:, :, :1], stats[:, :, 1:2]
    top = jnp.max(best, axis=0, keepdims=True)
    return top, jnp.sum(mass * jnp.exp(best - top), axis=0, keepdims=True)


def stats_kernel(marginal_ref, out_ref):
    marginal = marginal_ref[...]
    best = jnp.max(jnp.max(marginal, axis=0, keepdims=True), axis=2, keepdims=True)
    mass = jnp.sum(jnp.exp(marginal - best), axis=0, keepdims=True)
    mass = jnp.sum(mass, axis=2, keepdims=True)
    lane = lax.broadcasted_iota(jnp.int32, (1, 1, LANES), 2)
    out_ref[...] = jnp.broadcast_to(jnp.where(lane == 0, best, mass), out_ref.shape)


def final_kernel(stats_ref, marginal_ref, out_ref, evidence_ref, draws=0):
    top, mass = merged(stats_ref[...])
    total = top + jnp.log(mass)
    out_ref[...] = marginal_ref[...] - total
    evidence_ref[...] = total[0] - math.log(draws)


def body(fine_cross, fine_power, bin_widths, log_amps, delays, phases, chirps, proposal_log):
    shards, cores = lax.axis_size("draw"), lax.axis_size("bin")
    detectors, fine = fine_power.shape
    bins = bin_widths.shape[0]
    whole = log_amps.shape[1]
    draws = whole // cores
    widths = bin_widths.reshape(1, bins)
    turned, late = (
        [(i + int(shards * meet)) % shards for i in range(shards)] for meet in MEET
    )
    args = (fine_cross, fine_power, widths)
    sums = call(
        functools.partial(summary_kernel, grid=float(fine * shards)),
        jax.ShapeDtypeStruct((shards, 1, PAYLOAD), F32),
        *args, scratch=landing(args), pinned=True, flops=1 << 24, name="summary",
    )
    everyone = lax.all_to_all(sums, "draw", 0, 0, axis_index_groups=[turned], tiled=True)
    args = (
        widths, log_amps, delays, phases.reshape(1, whole), chirps.reshape(1, whole),
        proposal_log.reshape(1, whole),
    )
    terms = call(
        functools.partial(terms_kernel, grid=float(fine * shards), fine=fine, start=turned[0]),
        (
            jax.ShapeDtypeStruct((TSHIFT // 2 + TAIL, 2 * bins), BF16),
            jax.ShapeDtypeStruct((TSHIFT // 2 + TAIL, 2 * bins), BF16),
            jax.ShapeDtypeStruct((2 * detectors, bins, draws), F32),
            jax.ShapeDtypeStruct((16, draws), F32),
            jax.ShapeDtypeStruct((shards, bins), jnp.int32),
        ),
        *args, scratch=landing(args), pinned=True, flops=1 << 28, name="terms",
    )
    marginal = call(
        functools.partial(score_kernel, zero=turned.index(0)),
        jax.ShapeDtypeStruct((1, 1, draws), F32),
        everyone, *terms, flops=1 << 30, name="score",
    )
    marginals = lax.all_gather(marginal, "bin", axis=0, tiled=True)
    stat = call(
        stats_kernel, jax.ShapeDtypeStruct((shards, 1, LANES), F32), marginals, name="stats"
    )
    stats = lax.all_to_all(stat, "draw", 0, 0, axis_index_groups=[late], tiled=True)
    weights, evidence = call(
        lambda *refs: final_kernel(*refs, draws=whole * shards),
        (
            jax.ShapeDtypeStruct((cores, 1, draws), F32),
            jax.ShapeDtypeStruct((1, 1), F32),
        ),
        stats, marginals, name="final",
    )
    return weights.reshape(whole), evidence.reshape(1)


def solution(mesh):
    placed = (
        P("event", None, "draw"),
        P("event", "draw"),
        P("event"),
        P("event", "draw"),
        P("event", "draw"),
        P(("event", "draw")),
        P(("event", "draw")),
        P(("event", "draw")),
    )
    return jax.shard_map(
        body,
        mesh=mesh,
        in_specs=placed,
        out_specs=(P(("event", "draw")), P("event")),
        check_vma=False,
    )
```

```python
import functools
import math

import jax
import jax.numpy as jnp
import numpy as np
from jax import lax
from jax.experimental import pallas as pl
from jax.experimental.pallas import tpu as pltpu
from jax.sharding import PartitionSpec as P

TSHIFT = 2048
TIME_STEP = 0.125
LOG2 = math.log(2.0)
WIDE = 256
CHUNK = 128
TAIL = 16
STRIP = 128
LANES = 128
DET = 3
CHANNELS = 6
SPAN = 68
TERMS = 16
PAYLOAD = CHANNELS * SPAN + DET * TERMS
MEET = (0.75, 0.5)
VMEM = pl.BlockSpec(memory_space=pltpu.VMEM)
F32, BF16 = jnp.float32, jnp.bfloat16


def fit(function, terms):
    nodes = 0.125 * (1.0 + np.cos((np.arange(64) + 0.5) * np.pi / 64))
    basis = np.vander(nodes / 0.25, terms, increasing=True)
    found = np.linalg.lstsq(basis, function(np.sqrt(nodes)), rcond=None)[0]
    return [float(c) for c in found / 0.25 ** np.arange(terms)]


COS = fit(lambda r: np.cos(np.pi * r), 7)
SIN = fit(lambda r: np.sin(np.pi * r) / r, 6)


def horner(coefficients, x):
    total = jnp.full_like(x, coefficients[-1])
    for c in coefficients[-2::-1]:
        total = total * x + c
    return total


def turn(u):
    r = u - jnp.round(u)
    square = r * r
    cosine, sine = horner(COS, square), horner(SIN, square) * r
    twice = sine + sine
    return 1.0 - twice * sine, twice * cosine


def call(kernel, outs, *args, scratch=(), pinned=False, limit=24 << 20, flops=1 << 20, name=None):
    where = VMEM
    if pinned:
        where = pl.BlockSpec(memory_space=pltpu.HBM)
        args = [pltpu.with_memory_space_constraint(a, pltpu.HBM) for a in args]
    return pl.pallas_call(
        kernel,
        out_shape=outs,
        in_specs=[where] * len(args),
        out_specs=jax.tree.map(lambda _: VMEM, outs),
        scratch_shapes=scratch,
        compiler_params=pltpu.CompilerParams(vmem_limit_bytes=limit),
        cost_estimate=pl.CostEstimate(flops=flops, bytes_accessed=1 << 20, transcendentals=0),
        name=name,
    )(*args)


def landing(args):
    return [pltpu.VMEM(a.shape, a.dtype) for a in args] + [pltpu.SemaphoreType.DMA((len(args),))]


def fetch(sources, targets, semaphores):
    copies = [
        pltpu.make_async_copy(source, target, semaphores.at[i])
        for i, (source, target) in enumerate(zip(sources, targets))
    ]
    for copy in copies:
        copy.start()
    return copies


def shifted(x, amount):
    for bit in range(LANES.bit_length() - 1):
        x = jnp.where((amount >> bit) & 1 == 1, pltpu.roll(x, 1 << bit, 1), x)
    return x


def series():
    return [
        (-4.0 * c * math.comb(n, j), n - j, j)
        for n, c in ((2, 1.0), (4, -1.0 / 3), (6, 2.0 / 45))
        for j in range(n + 1)
    ]


def powers(x, count):
    found = [None, x]
    while len(found) <= count:
        found.append(found[-1] * x)
    return found


def monomial(left, right, i, j):
    if i and j:
        return left[i] * right[j]
    return left[i] if i else right[j]


def edges(widths):
    wide = widths.astype(F32)
    bins = wide.shape[1]
    before = lax.broadcasted_iota(jnp.int32, (bins, bins), 0)
    mine = lax.broadcasted_iota(jnp.int32, (bins, bins), 1)
    ones = jnp.where(before <= mine, 1.0, 0.0).astype(BF16)
    rows = jnp.broadcast_to(wide, (16, bins)).astype(BF16)
    upper = jnp.dot(rows, ones, preferred_element_type=F32)[:1]
    return wide, upper


def split(x):
    high = x.astype(BF16)
    return high, (x - high.astype(F32)).astype(BF16)


def summary_kernel(
    cross_in, power_in, widths_in, out_ref, cross_ref, power_ref, widths_ref, sems, grid=0.0
):
    copies = fetch(
        (widths_in, cross_in, power_in), (widths_ref, cross_ref, power_ref), sems
    )
    copies[0].wait()
    fine, bins = power_ref.shape[1], widths_ref.shape[1]
    wide, upper = edges(widths_ref[...])
    lower = upper - wide
    first = (lax.axis_index("draw") * fine).astype(F32)
    at = lax.broadcasted_iota(jnp.int32, (fine, bins), 0).astype(F32) + first
    inside = (at >= lower) & (at < upper)
    up = jnp.where(inside, 2.0 * (at - lower) + 1.0, 0.0)
    down = jnp.where(inside, 2.0 * wide - up, 0.0)
    both_high, both_low = split(up * down)
    weights = jnp.concatenate([up.astype(BF16), down.astype(BF16), both_high, both_low], axis=1)
    for copy in copies[1:]:
        copy.wait()
    data = jnp.concatenate(
        [cross_ref[d] for d in range(DET)] + [power_ref[...], jnp.zeros((7, fine), F32)], axis=0
    )
    high = data.astype(BF16)
    rest = data - high.astype(F32)
    middle, low = split(rest)
    got = jnp.dot(
        jnp.concatenate([high, middle, low], axis=0), weights, preferred_element_type=F32
    )
    got = got[:16] + got[16:32] + got[32:]
    scale = 0.5 / wide
    end = got[:, :bins] * scale
    start = got[:, bins : 2 * bins] * scale
    mixed = (got[:, 2 * bins : 3 * bins] + got[:, 3 * bins :]) * (scale * scale)
    row = lax.broadcasted_iota(jnp.int32, (16, bins), 0)
    lane = lax.broadcasted_iota(jnp.int32, (16, bins), 1)
    merged = end + pltpu.roll(start, bins - 1, 1)
    passed = jnp.sum(jnp.where(upper <= first, 1, 0), axis=1, keepdims=True)
    table = shifted(merged, (bins + 1 - passed) % bins)
    width, x = wide * (1.0 / grid), upper * (1.0 / grid)
    slope = powers(math.pi * width, 6)
    bend = powers(0.5 * width * (x + (x - width)), 6)
    factors = [c * monomial(slope, bend, i, j) for c, i, j in series()]
    factors = jnp.concatenate(factors + [jnp.zeros((1, bins), F32)], axis=0)
    extra = jnp.zeros((TERMS, bins), F32)
    total = jnp.sum(data, axis=1, keepdims=True)
    for d in range(DET):
        each = jnp.sum(factors * mixed[6 + d : 7 + d], axis=1, keepdims=True)
        each = jnp.where(row[:, :1] == TERMS - 1, total[6 + d : 7 + d], each)
        extra = jnp.where(lane == row + (CHANNELS * SPAN % bins + d * TERMS), each, extra)
    tiles = [jnp.zeros((1, bins), F32)] * 4
    tiles[3] = jnp.sum(extra, axis=0, keepdims=True)
    lane = lane[:1]
    for c in range(CHANNELS):
        tile, off = divmod(c * SPAN, bins)
        line = pltpu.roll(table[c : c + 1], off, 1) if off else table[c : c + 1]
        tiles[tile] = tiles[tile] + jnp.where(lane >= off, line, 0.0)
        if off + SPAN > bins:
            tiles[tile + 1] = tiles[tile + 1] + jnp.where(lane < off, line, 0.0)
    for r, tile in enumerate(tiles):
        end = min((r + 1) * bins, PAYLOAD)
        out_ref[:, :, r * bins : end] = jnp.broadcast_to(
            tile[None, :, : end - r * bins], (out_ref.shape[0], 1, end - r * bins)
        )


def terms_kernel(
    widths_in, amps_in, delays_in, phases_in, chirps_in, prior_in,
    cos_ref, sin_ref, features_ref, flat_ref, place_ref,
    widths_ref, amps_ref, delays_ref, phases_ref, chirps_ref, prior_ref, sems,
    grid=0.0, fine=0, start=0,
):
    copies = fetch(
        (widths_in, amps_in, delays_in, phases_in, chirps_in, prior_in),
        (widths_ref, amps_ref, delays_ref, phases_ref, chirps_ref, prior_ref),
        sems,
    )
    copies[0].wait()
    wide, upper = edges(widths_ref[...])
    bins = wide.shape[1]
    draws = features_ref.shape[2]
    mine = pl.ds(pl.multiple_of(lax.axis_index("bin") * draws, draws), draws)
    member = lax.broadcasted_iota(jnp.int32, place_ref.shape, 0)
    source = (member + start) % place_ref.shape[0] * fine
    passed = jnp.sum(jnp.where(upper <= source.astype(F32), 1, 0), axis=1, keepdims=True)
    place_ref[...] = jnp.broadcast_to((passed + (bins - 1)) % bins, place_ref.shape)
    step = upper * (TIME_STEP / grid)
    near = lax.broadcasted_iota(jnp.int32, (CHUNK, bins), 0).astype(F32)
    near_cos, near_sin = turn(near * step)
    for first in range(0, TSHIFT // 2 + TAIL, CHUNK):
        size = min(CHUNK, TSHIFT // 2 + TAIL - first)
        rows = slice(first, first + size)
        far_cos, far_sin = turn(float(first) * step)
        here_cos, here_sin = near_cos[:size], near_sin[:size]
        cosine = here_cos * far_cos - here_sin * far_sin
        sine = here_sin * far_cos + here_cos * far_sin
        cos_ref[rows, :bins], cos_ref[rows, bins:] = split(cosine)
        sin_ref[rows, :bins], sin_ref[rows, bins:] = split(sine)
    tall = jnp.concatenate([upper, jnp.zeros((bins - 1, bins), F32)], axis=0).T
    x = tall[:, :1] * (1.0 / grid)
    for copy in copies[1:]:
        copy.wait()
    chirps = chirps_ref[:, mine]
    base = phases_ref[:, mine] * (0.5 / math.pi)
    common = base + (chirps * (0.5 / math.pi)) * (x * x)
    cos0, sin0 = turn(base)
    for d in range(DET):
        amp = jnp.exp(amps_ref[d : d + 1, mine])
        delay = delays_ref[d : d + 1, mine]
        cosine, sine = turn(x * delay + common)
        features_ref[2 * d] = amp * cosine
        features_ref[2 * d + 1] = amp * sine
        flat_ref[2 * d : 2 * d + 1] = amp * cos0
        flat_ref[2 * d + 1 : 2 * d + 2] = amp * sin0
    flat_ref[6:7] = prior_ref[:, mine]
    flat_ref[7:8] = chirps
    flat_ref[8 : 8 + DET] = delays_ref[:, mine]
    flat_ref[8 + DET :] = jnp.zeros((8 - DET, draws), F32)


def score_kernel(
    sums_ref, cos_ref, sin_ref, features_ref, flat_ref, place_ref, out_ref, zero=0,
):
    bins = features_ref.shape[1]
    draws = features_ref.shape[2]
    half = TSHIFT // 2
    place = place_ref[...]
    row = lax.broadcasted_iota(jnp.int32, place.shape, 0)
    lane = lax.broadcasted_iota(jnp.int32, place.shape, 1)
    tiles = [sums_ref[:, 0, r * bins : (r + 1) * bins] for r in range(3)]
    last = sums_ref[:, 0, 3 * bins : PAYLOAD]
    rest = jnp.zeros((last.shape[0], 4 * bins - PAYLOAD), F32)
    tiles.append(jnp.concatenate([last, rest], axis=1))
    lines, single = [], []
    for c in range(CHANNELS):
        tile, off = divmod(c * SPAN, bins)
        line = pltpu.roll(tiles[tile], bins - off, 1) if off else tiles[tile]
        if off + SPAN > bins:
            line = jnp.where(lane < bins - off, line, pltpu.roll(tiles[tile + 1], bins - off, 1))
        line = shifted(jnp.where(lane < SPAN, line, 0.0), place)
        single.append(line[zero : zero + 1, bins - 1 :])
        line = jnp.where((row == zero) & (lane == bins - 1), 0.0, line)
        lines.append(jnp.sum(line, axis=0, keepdims=True))
    tall = jnp.concatenate(lines + [jnp.zeros((bins - CHANNELS, bins), F32)], axis=0).T
    extra = jnp.sum(tiles[3], axis=0, keepdims=True)
    extra = [
        pltpu.roll(extra, bins - CHANNELS * SPAN % bins - d * TERMS, 1) for d in range(DET)
    ]
    extra = jnp.concatenate(extra + [jnp.zeros((8 - DET, bins), F32)], axis=0)
    chirp = powers(jnp.broadcast_to(flat_ref[7:8], (8, draws)), 6)
    delay = powers(flat_ref[8:], 6)
    power = jnp.broadcast_to(extra[:, TERMS - 1 : TERMS], (8, draws))
    for k, (_, i, j) in enumerate(series()):
        power = power + extra[:, k : k + 1] * monomial(delay, chirp, i, j)
    real = imag = None
    offset = flat_ref[6:7]
    for d in range(DET):
        a, b = tall[:, 2 * d : 2 * d + 1], tall[:, 2 * d + 1 : 2 * d + 2]
        cosine, sine = features_ref[2 * d], features_ref[2 * d + 1]
        re, im = a * cosine + b * sine, b * cosine - a * sine
        real = re if real is None else real + re
        imag = im if imag is None else imag + im
        cos0, sin0 = flat_ref[2 * d : 2 * d + 1], flat_ref[2 * d + 1 : 2 * d + 2]
        offset = offset + single[2 * d] * cos0 + single[2 * d + 1] * sin0
        offset = offset - (0.5 * power[d : d + 1]) * (cos0 * cos0 + sin0 * sin0)
    real, imag = (
        [jnp.concatenate([piece, piece], axis=0) for piece in split(part * (1.0 / LOG2))]
        for part in (real, imag)
    )

    def rotated(rows, columns):
        return (
            jnp.dot(ref[rows, :], part[0][:, columns], preferred_element_type=F32)
            + jnp.dot(ref[rows, :], part[1][:, columns], preferred_element_type=F32)
            for ref, part in ((cos_ref, real), (sin_ref, imag))
        )

    marginal = []
    for start in range(0, draws, WIDE):
        columns = slice(start, start + WIDE)
        even, odd = rotated(slice(half, half + TAIL), columns)
        earliest = (even - odd)[:1]
        top = total = None
        for first in range(0, half, STRIP):
            even, odd = rotated(slice(first, first + STRIP), columns)
            after, before = even + odd, even - odd
            if first == 0:
                at = lax.broadcasted_iota(jnp.int32, before.shape, 0)
                before = jnp.where(at == 0, earliest, before)
            after = after.reshape(STRIP // 8, 8, WIDE)
            before = before.reshape(STRIP // 8, 8, WIDE)
            peak = jnp.max(jnp.maximum(after, before), axis=0)
            if top is not None:
                peak = jnp.maximum(peak, top)
                total = total * jnp.exp2(top - peak)
            add = jnp.sum(jnp.exp2(after - peak[None]) + jnp.exp2(before - peak[None]), axis=0)
            total = add if total is None else total + add
            top = peak
        peak = jnp.max(top, axis=0, keepdims=True)
        total = jnp.sum(total * jnp.exp2(top - peak), axis=0, keepdims=True)
        marginal.append(peak * LOG2 + (jnp.log(total) - math.log(TSHIFT)))
    marginal = jnp.concatenate(marginal, axis=1) + offset
    out_ref[...] = marginal[None]


def merged(stats):
    best, mass = stats[:, :, :1], stats[:, :, 1:2]
    top = jnp.max(best, axis=0, keepdims=True)
    return top, jnp.sum(mass * jnp.exp(best - top), axis=0, keepdims=True)


def stats_kernel(marginal_ref, out_ref):
    marginal = marginal_ref[...]
    best = jnp.max(jnp.max(marginal, axis=0, keepdims=True), axis=2, keepdims=True)
    mass = jnp.sum(jnp.exp(marginal - best), axis=0, keepdims=True)
    mass = jnp.sum(mass, axis=2, keepdims=True)
    lane = lax.broadcasted_iota(jnp.int32, (1, 1, LANES), 2)
    out_ref[...] = jnp.broadcast_to(jnp.where(lane == 0, best, mass), out_ref.shape)


def final_kernel(stats_ref, marginal_ref, out_ref, evidence_ref, draws=0):
    top, mass = merged(stats_ref[...])
    total = top + jnp.log(mass)
    out_ref[...] = marginal_ref[...] - total
    evidence_ref[...] = total[0] - math.log(draws)


def body(fine_cross, fine_power, bin_widths, log_amps, delays, phases, chirps, proposal_log):
    shards, cores = lax.axis_size("draw"), lax.axis_size("bin")
    detectors, fine = fine_power.shape
    bins = bin_widths.shape[0]
    whole = log_amps.shape[1]
    draws = whole // cores
    widths = bin_widths.reshape(1, bins)
    turned, late = (
        [(i + int(shards * meet)) % shards for i in range(shards)] for meet in MEET
    )
    args = (fine_cross, fine_power, widths)
    sums = call(
        functools.partial(summary_kernel, grid=float(fine * shards)),
        jax.ShapeDtypeStruct((shards, 1, PAYLOAD), F32),
        *args, scratch=landing(args), pinned=True, flops=1 << 24, name="summary",
    )
    everyone = lax.all_to_all(sums, "draw", 0, 0, axis_index_groups=[turned], tiled=True)
    args = (
        widths, log_amps, delays, phases.reshape(1, whole), chirps.reshape(1, whole),
        proposal_log.reshape(1, whole),
    )
    terms = call(
        functools.partial(terms_kernel, grid=float(fine * shards), fine=fine, start=turned[0]),
        (
            jax.ShapeDtypeStruct((TSHIFT // 2 + TAIL, 2 * bins), BF16),
            jax.ShapeDtypeStruct((TSHIFT // 2 + TAIL, 2 * bins), BF16),
            jax.ShapeDtypeStruct((2 * detectors, bins, draws), F32),
            jax.ShapeDtypeStruct((16, draws), F32),
            jax.ShapeDtypeStruct((shards, bins), jnp.int32),
        ),
        *args, scratch=landing(args), pinned=True, flops=1 << 28, name="terms",
    )
    marginal = call(
        functools.partial(score_kernel, zero=turned.index(0)),
        jax.ShapeDtypeStruct((1, 1, draws), F32),
        everyone, *terms, flops=1 << 30, name="score",
    )
    marginals = lax.all_gather(marginal, "bin", axis=0, tiled=True)
    stat = call(
        stats_kernel, jax.ShapeDtypeStruct((shards, 1, LANES), F32), marginals, name="stats"
    )
    stats = lax.all_to_all(stat, "draw", 0, 0, axis_index_groups=[late], tiled=True)
    weights, evidence = call(
        lambda *refs: final_kernel(*refs, draws=whole * shards),
        (
            jax.ShapeDtypeStruct((cores, 1, draws), F32),
            jax.ShapeDtypeStruct((1, 1), F32),
        ),
        stats, marginals, name="final",
    )
    return weights.reshape(whole), evidence.reshape(1)


def solution(mesh):
    placed = (
        P("event", None, "draw"),
        P("event", "draw"),
        P("event"),
        P("event", "draw"),
        P("event", "draw"),
        P(("event", "draw")),
        P(("event", "draw")),
        P(("event", "draw")),
    )
    return jax.shard_map(
        body,
        mesh=mesh,
        in_specs=placed,
        out_specs=(P(("event", "draw")), P("event")),
        check_vma=False,
    )
```
